512 devices in a mesh: gx: 32 (over x_lo, z, core), yz: 16 (over x_hi, y).
Axes of the slice: x: 4 (x_hi: 2, x_lo: 2; x = x_hi * 2 + x_lo), y: 8, z: 8, core: 2. Of those that a mesh axis runs over, the one named last changes fastest.
Arguments:
- leaf_moments: bfloat16 [256, 128, 256], P('gx', 'yz'), may hold values from -6 to 6
- leaf_list: int32 [256, 128, 16], P('gx', 'yz'), may hold values from 0 to 288
- leaf_op: int32 [256, 128, 16], P('gx', 'yz'), may hold values from 0 to 15
- leaf_parent: int32 [256, 128], P('gx', 'yz'), may hold values from 0 to 127, as said below
- leaf_octant: int32 [256, 128], P('gx', 'yz'), may hold values from 0 to 7, as said below
- parent_list: int32 [32, 128, 8], P('gx', 'yz'), may hold values from 0 to 639
- parent_op: int32 [32, 128, 8], P('gx', 'yz'), may hold values from 0 to 15
- operators: bfloat16 [16, 256, 256], replicated, may hold values from -0.09375 to 0.09375
- shift_up: bfloat16 [8, 256, 256], replicated, may hold values from -0.125 to 0.125
- density: bfloat16 [8192, 128, 128], P(('gx', 'yz')), may hold values from -6 to 6
- nearby_coulomb_kernel: bfloat16 [8, 128, 128], replicated, may hold values from -0.1875 to 0.1875
- near_src: int32 [8192, 16], P(('gx', 'yz')), may hold values from 0 to 15
- near_kind: int32 [8192, 16], P(('gx', 'yz')), may hold values from 0 to 7
- near_count: int32 [8192], P(('gx', 'yz')), may hold values from 1 to 16
- eval_rows: float32 [128, 16], replicated, may hold values from -1.5 to 1.5
- eval_cols: float32 [16, 128], replicated, may hold values from -1.5 to 1.5
Outputs:
- coulomb: bfloat16 [8192, 128, 128], P(('gx', 'yz'))
The draws below stay inside these ranges and needn't reach their ends.
Inputs may be any that keep to these rules, and one draw needn't show every extreme that they name: `leaf_parent`: within each column of leaf blocks (a // 8 fixed) every coarse box number is named by exactly 8 leaves. `leaf_octant`: the 8 leaves of one coarse box have 8 different octants.
All inputs are finite; a program needn't handle non-finite values.
Results may differ from the reference program's by a relative error of at most 0.0026.
Values may be sent and summed in bfloat16 or wider, within the bound.
No kernel may reach another device: no remote copies, remote signals or barrier semaphores. Data moves between devices by JAX's collectives and lax.ppermute only.
A program may use at most 64 MiB of HBM per device.

```python
import jax
import jax.numpy as jnp
from jax import lax

P_SIZE = 256
HARM = 16
SHELL = 128
LEAF_SIDE = 8
LIST = 16
PLIST = 8
OPS = 16
KINDS = 8
NEAR = 16
BOX_TILE = 4
GXB = 256
YZB = 128
PAR_COL = 128
TILES_DEV = 16
TILES = 8192
N_GX = 32
N_YZ = 16


def family_codes(key):
    column_count = GXB // LEAF_SIDE
    keys = jax.random.split(jax.random.fold_in(key, 11), column_count)
    orders = jax.vmap(lambda one_key: jax.random.permutation(one_key, 8 * PAR_COL))(keys)
    return orders.reshape(GXB, YZB).astype(jnp.int32)


def draw_leaf_parent(key, part):
    return family_codes(key) // 8


def draw_leaf_octant(key, part):
    return family_codes(key) % 8


def draw_near_count(key, part):
    blocks_count = TILES // TILES_DEV
    limits = jax.random.randint(jax.random.fold_in(key, 1), (blocks_count,), NEAR // 4, NEAR + 1)
    picked = jax.random.randint(jax.random.fold_in(key, 2), (), 0, blocks_count)
    limits = jnp.where(jnp.arange(blocks_count) == picked, NEAR, limits)
    counts = jax.random.randint(jax.random.fold_in(key, 3), (blocks_count, TILES_DEV), 1, limits[:, None] + 1)
    counts = jnp.where(jnp.arange(TILES_DEV)[None, :] == 0, limits[:, None], counts)
    return counts.reshape(TILES).astype(jnp.int32)


def place_ends(result, rng, smallest, top_value):
    longest = result.shape.index(max(result.shape))
    spots = []
    for shift in (0, 1):
        where = [jax.random.randint(jax.random.fold_in(rng, axis), (), 0, length) for axis, length in enumerate(result.shape)]
        where[longest] = (where[longest] + shift) % result.shape[longest]
        spots.append(tuple(where))
    return result.at[spots[0]].set(smallest).at[spots[1]].set(top_value)


def shard_levels(rng, shape, shards, low, top_value):
    factor_of = 1.0
    for dim, parts in shards:
        heights = jax.random.uniform(jax.random.fold_in(jax.random.fold_in(rng, 6), dim), (parts,), jnp.float32, low / len(shards), top_value / len(shards))
        factor_of = factor_of * jnp.repeat(jnp.exp(heights), shape[dim] // parts).reshape((-1,) + (1,) * (len(shape) - 1 - dim))
    return factor_of


def bell_draw(key, dims, scale, reach, shards=(), kind=jnp.bfloat16):
    values = scale * jax.random.normal(key, dims, jnp.float32)
    if shards:
        values = values * shard_levels(key, dims, shards, -0.22, 0.18)
    return jnp.clip(values, -reach, reach).astype(kind)


def setup_inputs(seed: int = 0) -> dict:
    seeds = jax.random.split(jax.random.key(seed), 17)
    leaf_moments = bell_draw(seeds[0], (GXB, YZB, P_SIZE), 1.0, 6.0, ((0, 32), (1, 16)))
    leaf_list = place_ends(jax.random.randint(seeds[1], (GXB, YZB, LIST), 0, (2 * LEAF_SIDE + 1) * (2 * LEAF_SIDE + 1)), jax.random.fold_in(seeds[1], 1), 0, ((2 * LEAF_SIDE + 1) * (2 * LEAF_SIDE + 1)) - 1).astype(jnp.int32)
    leaf_op = place_ends(jax.random.randint(seeds[2], (GXB, YZB, LIST), 0, OPS), jax.random.fold_in(seeds[2], 1), 0, OPS - 1).astype(jnp.int32)
    leaf_parent = draw_leaf_parent(jax.random.fold_in(seeds[16], 71), 0)
    leaf_octant = draw_leaf_octant(jax.random.fold_in(seeds[16], 71), 0)
    parent_list = place_ends(jax.random.randint(seeds[5], (N_GX, PAR_COL, PLIST), 0, 5 * PAR_COL), jax.random.fold_in(seeds[5], 1), 0, (5 * PAR_COL) - 1).astype(jnp.int32)
    parent_op = place_ends(jax.random.randint(seeds[6], (N_GX, PAR_COL, PLIST), 0, OPS), jax.random.fold_in(seeds[6], 1), 0, OPS - 1).astype(jnp.int32)
    operators = bell_draw(seeds[7], (OPS, P_SIZE, P_SIZE), (P_SIZE * LIST) ** -0.5, 0.09375)
    shift_up = bell_draw(seeds[8], (8, P_SIZE, P_SIZE), (8 * P_SIZE) ** -0.5, 0.125)
    density = bell_draw(seeds[9], (TILES, SHELL, SHELL), 1.0, 6.0, ((0, 512),))
    nearby_coulomb_kernel = bell_draw(seeds[10], (KINDS, SHELL, SHELL), (SHELL * NEAR // 2) ** -0.5, 0.1875)
    near_src = place_ends(jax.random.randint(seeds[11], (TILES, NEAR), 0, TILES_DEV), jax.random.fold_in(seeds[11], 1), 0, TILES_DEV - 1).astype(jnp.int32)
    near_kind = place_ends(jax.random.randint(seeds[12], (TILES, NEAR), 0, KINDS), jax.random.fold_in(seeds[12], 1), 0, KINDS - 1).astype(jnp.int32)
    near_count = draw_near_count(jax.random.fold_in(seeds[16], 71), 0)
    eval_rows = bell_draw(seeds[14], (SHELL, HARM), HARM ** -0.5, 1.5, (), jnp.float32)
    eval_cols = bell_draw(seeds[15], (HARM, SHELL), HARM ** -0.5, 1.5, (), jnp.float32)
    return {"leaf_moments": leaf_moments, "leaf_list": leaf_list, "leaf_op": leaf_op, "leaf_parent": leaf_parent, "leaf_octant": leaf_octant, "parent_list": parent_list, "parent_op": parent_op, "operators": operators, "shift_up": shift_up, "density": density, "nearby_coulomb_kernel": nearby_coulomb_kernel, "near_src": near_src, "near_kind": near_kind, "near_count": near_count, "eval_rows": eval_rows, "eval_cols": eval_cols}


def grouped_products(sources, op_index, operators):
    summed = jnp.zeros(sources[0].shape, jnp.float32)
    for operator_number in range(operators.shape[0]):
        collected_tiles = jnp.zeros(sources[0].shape, jnp.float32)
        for slot_number in range(len(sources)):
            picked = (op_index[..., slot_number] == operator_number)[..., None]
            collected_tiles = collected_tiles + jnp.where(picked, sources[slot_number].astype(jnp.float32), jnp.float32(0.0))
        summed = summed + jnp.einsum("...p,pq->...q", collected_tiles, operators[operator_number].astype(jnp.float32), precision=lax.Precision.HIGHEST)
    return summed


def reference(leaf_moments, leaf_list, leaf_op, leaf_parent, leaf_octant, parent_list, parent_op, operators, shift_up, density, nearby_coulomb_kernel, near_src, near_kind, near_count, eval_rows, eval_cols):
    code_span = 2 * LEAF_SIDE + 1
    index_first = lax.broadcasted_iota(jnp.int32, (GXB, YZB), 0)
    index_second = lax.broadcasted_iota(jnp.int32, (GXB, YZB), 1)
    sources = []
    for slot_number in range(LIST):
        slot_code = leaf_list[:, :, slot_number]
        row_first = (index_first + slot_code // code_span - LEAF_SIDE) % GXB
        row_second = (index_second + slot_code % code_span - LEAF_SIDE) % YZB
        sources.append(leaf_moments[row_first, row_second])
    far_local = grouped_products(sources, leaf_op, operators)
    moments_wide = leaf_moments.astype(jnp.float32)
    translated = jnp.zeros((GXB, YZB, P_SIZE), jnp.float32)
    for octant in range(8):
        chosen = jnp.where((leaf_octant == octant)[..., None], moments_wide, jnp.float32(0.0))
        translated = translated + jnp.einsum("xyp,pq->xyq", chosen, shift_up[octant].astype(jnp.float32), precision=lax.Precision.HIGHEST)
    segment = (index_first // LEAF_SIDE) * PAR_COL + leaf_parent
    parent_moments = jax.ops.segment_sum(translated.reshape(GXB * YZB, P_SIZE), segment.reshape(GXB * YZB), num_segments=N_GX * PAR_COL)
    parent_moments = parent_moments.reshape(N_GX, PAR_COL, P_SIZE).astype(jnp.bfloat16)
    column_index = lax.broadcasted_iota(jnp.int32, (N_GX, PAR_COL), 0)
    coarse_sources = []
    for slot_number in range(PLIST):
        slot_code = parent_list[:, :, slot_number]
        source_column = (column_index + slot_code // PAR_COL - 2) % N_GX
        coarse_sources.append(parent_moments[source_column, slot_code % PAR_COL])
    parent_locals = grouped_products(coarse_sources, parent_op, operators).astype(jnp.bfloat16)
    parent_rows = parent_locals[index_first // LEAF_SIDE, leaf_parent].astype(jnp.float32)
    lowered = jnp.zeros((GXB, YZB, P_SIZE), jnp.float32)
    for octant in range(8):
        chosen = jnp.where((leaf_octant == octant)[..., None], parent_rows, jnp.float32(0.0))
        lowered = lowered + jnp.einsum("xyp,qp->xyq", chosen, shift_up[octant].astype(jnp.float32), precision=lax.Precision.HIGHEST)
    leaf_local = far_local + lowered
    blocks = leaf_local.reshape(N_GX, LEAF_SIDE, N_YZ, LEAF_SIDE, P_SIZE).transpose(0, 2, 1, 3, 4)
    blocks = blocks.reshape(TILES, BOX_TILE, HARM, HARM)
    left_half = jnp.einsum("rai,trij->traj", eval_rows.reshape(BOX_TILE, SHELL // BOX_TILE, HARM), blocks, precision=lax.Precision.HIGHEST)
    left_half = left_half.reshape(TILES, SHELL, HARM)
    far_tiles = jnp.einsum("taj,jb->tab", left_half, eval_cols, precision=lax.Precision.HIGHEST)
    tile_base = (jnp.arange(TILES, dtype=jnp.int32) // TILES_DEV) * TILES_DEV
    nearby_tile_list = jnp.zeros((TILES, SHELL, SHELL), jnp.float32)
    for interaction_kind in range(KINDS):
        collected_tiles = jnp.zeros((TILES, SHELL, SHELL), jnp.float32)
        for slot_number in range(NEAR):
            taken = (near_kind[:, slot_number] == interaction_kind) & (slot_number < near_count)
            paired_shell = density[tile_base + near_src[:, slot_number]].astype(jnp.float32)
            collected_tiles = collected_tiles + jnp.where(taken[:, None, None], paired_shell, jnp.float32(0.0))
        nearby_tile_list = nearby_tile_list + jnp.einsum("zf,pfo->pzo", nearby_coulomb_kernel[interaction_kind].astype(jnp.float32), collected_tiles, precision=lax.Precision.HIGHEST)
    return (nearby_tile_list + far_tiles).astype(jnp.bfloat16)
```

```python
import functools

import jax
import jax.numpy as jnp
from jax import lax
from jax.experimental import pallas as pl
from jax.experimental.pallas import tpu as pltpu
from jax.sharding import PartitionSpec as P

BF16 = jnp.bfloat16
F32 = jnp.float32
LEAVES = 64
ROWS = 72
COEFFS = 256
PARENTS = 128
OPS = 16
OCTANTS = 8
SLOTS = 16
PSLOTS = 8
MIB = 1024 * 1024


def dot(a, b):
    return jnp.dot(a, b, preferred_element_type=F32)


def dot_rows(a, b):
    return lax.dot_general(a, b, (((1,), (1,)), ((), ())), preferred_element_type=F32)


def one_hot(labels, positions):
    return jnp.where(labels == positions, 1.0, 0.0).astype(BF16)


def halves(x):
    high = x.astype(BF16)
    return high, (x - high.astype(F32)).astype(BF16)


def near_kernel(src_ref, kind_ref, count_ref, density_ref, kinds_ref, out_ref, products):
    kinds_count, side, _ = kinds_ref.shape
    tiles = density_ref.shape[0]
    stacked = kinds_ref[...].reshape(kinds_count * side, side)

    @pl.loop(0, tiles // 2)
    def _(pair):
        both = jnp.concatenate([density_ref[2 * pair], density_ref[2 * pair + 1]], axis=1)
        made = dot(stacked, both)
        for half in range(2):
            products[2 * pair + half] = made[:, half * side : (half + 1) * side].reshape(
                kinds_count, side, side
            )

    @pl.loop(0, tiles)
    def _(tile):
        def add(slot, total):
            return total + products[src_ref[tile, slot], kind_ref[tile, slot]]

        out_ref[tile] = lax.fori_loop(
            0, count_ref[tile], add, jnp.zeros((side, side), F32)
        )


def parent_kernel(own_ref, gathered_ref, shift_ref, window_ref, parents_ref):
    peers = gathered_ref.shape[0]
    sources = gathered_ref[:, :LEAVES, :].reshape(peers * LEAVES, COEFFS)
    labels = []
    for peer in range(peers):
        numbers = gathered_ref[peer, LEAVES : LEAVES + 8, :].astype(F32)
        labels.append(numbers[0:1, :LEAVES] + numbers[1:2, :LEAVES] * float(PARENTS))
    labels = jnp.concatenate(labels, axis=1).astype(jnp.int32)
    positions = lax.broadcasted_iota(jnp.int32, (PARENTS, peers * LEAVES), 0)
    total = jnp.zeros((PARENTS, COEFFS), F32)
    for octant in range(OCTANTS):
        chosen = one_hot(labels, positions + octant * PARENTS)
        total = total + dot(dot(chosen, sources).astype(BF16), shift_ref[octant])
    parents = total.astype(BF16)
    parents_ref[...] = parents
    window_ref[:PARENTS, :] = parents
    own = own_ref[0]
    for place in range(3):
        peer = lax.rem(own + place + peers - 1, peers)
        window_ref[PARENTS + place * LEAVES : PARENTS + (place + 1) * LEAVES, :] = gathered_ref[
            peer, :LEAVES, :
        ]


def op_rows(numbers, first, slots):
    rows = [numbers[first + slot : first + slot + 1, :] for slot in range(slots)]
    return jnp.concatenate(rows, axis=1)


def by_operator(rows, picked, slots):
    shape = (LEAVES, slots * LEAVES)
    same = (lax.broadcasted_iota(jnp.int32, shape, 1) % LEAVES) == lax.broadcasted_iota(
        jnp.int32, shape, 0
    )
    diagonal = jnp.where(same, rows, -1.0)
    chosen = jnp.concatenate([one_hot(diagonal, float(op)) for op in range(OPS)], axis=0)
    return dot(chosen, picked)


def final_kernel(
    codes_ref,
    ops_ref,
    eye_ref,
    pick_ref,
    lists_ref,
    own_ref,
    before_ref,
    after_ref,
    before2_ref,
    after2_ref,
    operators_ref,
    shift_ref,
    left_ref,
    right_high_ref,
    right_low_ref,
    near_ref,
    out_ref,
    staged,
):
    codes = codes_ref[...]
    peers = lists_ref.shape[0]

    blocks = 3 * LEAVES
    place = lax.broadcasted_iota(jnp.int32, (LEAVES, blocks), 1)
    picked = jnp.zeros((SLOTS * LEAVES, COEFFS), F32)
    for number, ref in enumerate((before_ref, own_ref, after_ref)):
        chosen = jnp.concatenate(
            [one_hot(codes[:, s : s + 1], place + number * blocks) for s in range(SLOTS)], axis=0
        )
        picked = picked + dot(chosen, ref[PARENTS:, :])
    leaf_rows = op_rows(dot_rows(eye_ref[...], ops_ref[...]), 0, SLOTS)
    leaf_sums = by_operator(leaf_rows, picked.astype(BF16), SLOTS)

    parent_of = codes[:, SLOTS : SLOTS + 1]
    octant_of = codes[:, SLOTS + 1 : SLOTS + 2]
    owner = one_hot(parent_of // 8, lax.broadcasted_iota(jnp.int32, (LEAVES, peers), 1))
    entries = dot(owner, lists_ref[...])
    lane = lax.broadcasted_iota(jnp.int32, (LEAVES, COEFFS), 1)
    entries = jnp.where((lane % LEAVES) // 8 == parent_of % 8, entries, 0.0).astype(BF16)
    by_leaf = dot_rows(entries, pick_ref[...]).astype(jnp.int32)
    by_slot = dot_rows(pick_ref[...], entries)
    column = lax.broadcasted_iota(jnp.int32, (LEAVES, PARENTS), 1)
    coarse = jnp.zeros((PSLOTS * LEAVES, COEFFS), F32)
    for number, ref in enumerate((before2_ref, before_ref, own_ref, after_ref, after2_ref)):
        chosen = jnp.concatenate(
            [one_hot(by_leaf[:, s : s + 1], column + number * PARENTS) for s in range(PSLOTS)],
            axis=0,
        )
        coarse = coarse + dot(chosen, ref[:PARENTS, :])
    coarse_rows = op_rows(by_slot, PSLOTS, PSLOTS)
    coarse_sums = by_operator(coarse_rows, coarse.astype(BF16), PSLOTS)

    leaf_high, leaf_low = halves(leaf_sums)
    coarse_high, coarse_low = halves(coarse_sums)
    total = jnp.zeros((4 * LEAVES, COEFFS), F32)
    for op in range(OPS):
        rows = slice(op * LEAVES, (op + 1) * LEAVES)
        stacked = jnp.concatenate(
            [leaf_high[rows], leaf_low[rows], coarse_high[rows], coarse_low[rows]], axis=0
        )
        total = total + dot(stacked, operators_ref[op])
    local = total[:LEAVES] + total[LEAVES : 2 * LEAVES]
    coarse_local = total[2 * LEAVES : 3 * LEAVES] + total[3 * LEAVES :]
    coarse_local = coarse_local.astype(BF16).astype(F32)
    for octant in range(OCTANTS):
        chosen = jnp.where(octant_of == octant, coarse_local, 0.0).astype(BF16)
        local = local + dot_rows(chosen, shift_ref[octant])

    high, low = halves(local)
    spread = dot(jnp.concatenate([high, low], axis=0), right_high_ref[...])
    spread = spread[:LEAVES] + spread[LEAVES:] + dot(high, right_low_ref[...])
    harmonics = 16
    side = out_ref.shape[1]
    for row in range(harmonics):
        staged[pl.ds(row, LEAVES, stride=harmonics), :] = spread[:, row * side : (row + 1) * side]
    left = left_ref[...]
    for pair in range(out_ref.shape[0] // 2):
        parts = []
        for tile in (2 * pair, 2 * pair + 1):
            tile_high, tile_low = halves(staged[tile * LEAVES : (tile + 1) * LEAVES, :])
            parts.append(jnp.concatenate([tile_high, tile_low, tile_high, tile_low], axis=0))
        far = dot(left, jnp.concatenate(parts, axis=1))
        for half, tile in enumerate((2 * pair, 2 * pair + 1)):
            out_ref[tile] = (near_ref[tile] + far[:, half * side : (half + 1) * side]).astype(BF16)


VMEM = pl.BlockSpec(memory_space=pltpu.VMEM)
SMEM = pl.BlockSpec(memory_space=pltpu.SMEM)


def near_call(near_src, near_kind, near_count, density, kinds):
    tiles, side, _ = density.shape
    return pl.pallas_call(
        near_kernel,
        name="near",
        out_shape=jax.ShapeDtypeStruct((tiles, side, side), F32),
        in_specs=[SMEM, SMEM, SMEM, VMEM, VMEM],
        out_specs=VMEM,
        scratch_shapes=[pltpu.VMEM((tiles, kinds.shape[0], side, side), F32)],
        compiler_params=pltpu.CompilerParams(vmem_limit_bytes=20 * MIB),
        cost_estimate=pl.CostEstimate(
            flops=4 * 10**9, bytes_accessed=2 * MIB, transcendentals=0
        ),
    )(near_src, near_kind, near_count, density, kinds)


def parent_call(own, gathered, shift_up):
    return pl.pallas_call(
        parent_kernel,
        name="parents",
        out_shape=(
            jax.ShapeDtypeStruct((PARENTS + 3 * LEAVES, COEFFS), BF16),
            jax.ShapeDtypeStruct((PARENTS, COEFFS), BF16),
        ),
        in_specs=[SMEM, VMEM, VMEM],
        out_specs=(VMEM, VMEM),
        compiler_params=pltpu.CompilerParams(vmem_limit_bytes=12 * MIB),
        cost_estimate=pl.CostEstimate(
            flops=2 * 10**9, bytes_accessed=2 * MIB, transcendentals=0
        ),
    )(own, gathered, shift_up)


def final_call(*operands):
    near = operands[-1]
    return pl.pallas_call(
        final_kernel,
        name="final",
        out_shape=jax.ShapeDtypeStruct(near.shape, BF16),
        in_specs=[VMEM] * len(operands),
        out_specs=VMEM,
        scratch_shapes=[pltpu.VMEM((LEAVES * 16, near.shape[1]), F32)],
        compiler_params=pltpu.CompilerParams(vmem_limit_bytes=32 * MIB),
        cost_estimate=pl.CostEstimate(
            flops=4 * 10**9, bytes_accessed=8 * MIB, transcendentals=0
        ),
    )(*operands)


def payload(leaf_moments, leaf_parent, leaf_octant, parent_list, parent_op):
    coarse = parent_list.reshape(1, LEAVES)
    rest = jnp.zeros((1, COEFFS - LEAVES), jnp.int32)
    numbers = jnp.concatenate(
        [
            jnp.concatenate([leaf_parent.reshape(1, LEAVES), rest], axis=1),
            jnp.concatenate([leaf_octant.reshape(1, LEAVES), rest], axis=1),
            jnp.concatenate(
                [
                    coarse // PARENTS,
                    coarse % PARENTS,
                    parent_op.reshape(1, LEAVES),
                    jnp.zeros((1, LEAVES), jnp.int32),
                ],
                axis=1,
            ),
            jnp.zeros((ROWS - LEAVES - 3, COEFFS), jnp.int32),
        ],
        axis=0,
    ).astype(BF16)
    return jnp.concatenate([leaf_moments.reshape(LEAVES, COEFFS), numbers], axis=0)


def leaf_codes(leaf_list, leaf_parent, leaf_octant):
    side = leaf_list.shape[0]
    span = 2 * side + 1
    first = lax.broadcasted_iota(jnp.int32, leaf_list.shape, 0) + leaf_list // span
    second = lax.broadcasted_iota(jnp.int32, leaf_list.shape, 1) + leaf_list % span
    window = (
        (first // side) * (3 * LEAVES)
        + (second // side) * LEAVES
        + (first % side) * side
        + second % side
    )
    return jnp.concatenate(
        [
            window.reshape(LEAVES, SLOTS),
            leaf_parent.reshape(LEAVES, 1),
            leaf_octant.reshape(LEAVES, 1),
        ],
        axis=1,
    )


def split(x):
    high = lax.reduce_precision(x, 8, 7)
    return high.astype(BF16), (x - high).astype(BF16)


def eval_tables(eval_rows, eval_cols):
    side, harmonics = eval_rows.shape
    rows = jnp.tile(eval_rows, (1, 4))
    shape = rows.shape
    rows = jnp.where(
        lax.broadcasted_iota(jnp.int32, shape, 0) // (side // 4)
        == lax.broadcasted_iota(jnp.int32, shape, 1) // harmonics,
        rows,
        0.0,
    )
    high, low = split(rows)
    left = jnp.concatenate([high, high, low, low], axis=1)
    shape = (harmonics * harmonics, harmonics * side)
    columns = jnp.where(
        lax.broadcasted_iota(jnp.int32, shape, 0) // harmonics
        == lax.broadcasted_iota(jnp.int32, shape, 1) // side,
        jnp.tile(eval_cols, (harmonics, harmonics)),
        0.0,
    )
    return left, *split(columns)


def pick_table():
    shape = (16, COEFFS)
    row = lax.broadcasted_iota(jnp.int32, shape, 0)
    lane = lax.broadcasted_iota(jnp.int32, shape, 1)
    part, slot = lane // LEAVES, lane % PSLOTS
    value = jnp.where(part == 0, 128.0, 1.0)
    hit = (part < 2) & (row == slot) | (part == 2) & (row == slot + PSLOTS)
    return jnp.where(hit, value, 0.0).astype(BF16)


def shifted(value, axis, distance):
    peers = lax.axis_size(axis)
    return lax.ppermute(value, axis, [(i, (i + distance) % peers) for i in range(peers)])


def body(
    leaf_moments,
    leaf_list,
    leaf_op,
    leaf_parent,
    leaf_octant,
    parent_list,
    parent_op,
    operators,
    shift_up,
    density,
    nearby_coulomb_kernel,
    near_src,
    near_kind,
    near_count,
    eval_rows,
    eval_cols,
):
    own = lax.axis_index("yz").astype(jnp.int32).reshape(1)
    sent = payload(leaf_moments, leaf_parent, leaf_octant, parent_list[0], parent_op[0])
    copies = jnp.broadcast_to(sent, (lax.axis_size("yz"), *sent.shape))
    gathered = lax.all_to_all(copies, "yz", split_axis=0, concat_axis=0, tiled=True)

    near = near_call(near_src, near_kind, near_count, density, nearby_coulomb_kernel)
    codes = leaf_codes(leaf_list, leaf_parent, leaf_octant)
    left, right_high, right_low = eval_tables(eval_rows, eval_cols)

    window, parents = parent_call(own, gathered, shift_up)
    before = shifted(window, "gx", 1)
    after = shifted(window, "gx", -1)
    before2 = shifted(parents, "gx", 2)
    after2 = shifted(parents, "gx", -2)
    return final_call(
        codes,
        leaf_op.reshape(LEAVES, SLOTS).astype(BF16),
        jnp.eye(SLOTS, dtype=BF16),
        pick_table(),
        gathered[:, LEAVES + 2, :],
        window,
        before,
        after,
        before2,
        after2,
        operators,
        shift_up,
        left,
        right_high,
        right_low,
        near,
    )


def solution(mesh):
    in_specs = (
        P("gx", "yz", None),
        P("gx", "yz", None),
        P("gx", "yz", None),
        P("gx", "yz"),
        P("gx", "yz"),
        P("gx", "yz", None),
        P("gx", "yz", None),
        P(),
        P(),
        P(("gx", "yz"), None, None),
        P(),
        P(("gx", "yz"), None),
        P(("gx", "yz"), None),
        P(("gx", "yz")),
        P(),
        P(),
    )
    out_specs = P(("gx", "yz"), None, None)
    return jax.shard_map(body, mesh=mesh, in_specs=in_specs, out_specs=out_specs, check_vma=False)
```

```python
import functools

import jax
import jax.numpy as jnp
from jax import lax
from jax.experimental import pallas as pl
from jax.experimental.pallas import tpu as pltpu
from jax.sharding import PartitionSpec as P

BF16 = jnp.bfloat16
F32 = jnp.float32
LEAVES = 64
ROWS = 136
COEFFS = 256
HALF = 128
BLOCKS = 3 * LEAVES
PARENTS = 128
OPS = 16
OCTANTS = 8
SLOTS = 16
PSLOTS = 8
MIB = 1024 * 1024


def dot(a, b):
    return jnp.dot(a, b, preferred_element_type=F32)


def dot_rows(a, b):
    return lax.dot_general(a, b, (((1,), (1,)), ((), ())), preferred_element_type=F32)


def one_hot(labels, positions):
    return jnp.where(labels == positions, 1.0, 0.0).astype(BF16)


def halves(x):
    high = x.astype(BF16)
    return high, (x - high.astype(F32)).astype(BF16)


def near_field(src_ref, kind_ref, count_ref, density_ref, kinds_ref, out_ref, products):
    kinds_count, side, _ = kinds_ref.shape
    tiles = density_ref.shape[0]
    stacked = kinds_ref[...].reshape(kinds_count * side, side)

    @pl.loop(0, tiles // 2)
    def _(pair):
        both = jnp.concatenate([density_ref[2 * pair], density_ref[2 * pair + 1]], axis=1)
        made = dot(stacked, both)
        for half in range(2):
            products[2 * pair + half] = made[:, half * side : (half + 1) * side].reshape(
                kinds_count, side, side
            )

    @pl.loop(0, tiles)
    def _(tile):
        def add(slot, total):
            return total + products[src_ref[tile, slot], kind_ref[tile, slot]]

        out_ref[tile] = lax.fori_loop(
            0, count_ref[tile], add, jnp.zeros((side, side), F32)
        )


def payload_kernel(*refs):
    sources, out_ref, held, block, in_sem, out_sem = refs[:5], refs[5], refs[6:11], *refs[11:]
    fetches = [
        pltpu.make_async_copy(source, target, in_sem.at[number])
        for number, (source, target) in enumerate(zip(sources, held))
    ]
    for fetch in fetches:
        fetch.start()
    for fetch in fetches:
        fetch.wait()
    moments_ref, parent_ref, octant_ref, list_ref, op_ref = held
    coarse = list_ref[...]
    numbers = jnp.concatenate(
        [parent_ref[...], octant_ref[...], coarse >> 7, coarse & 127, op_ref[...]], axis=0
    )
    count, side = numbers.shape
    lane = lax.broadcasted_iota(jnp.int32, (side, LEAVES), 1)
    spread = dot(
        numbers.astype(F32).astype(BF16),
        one_hot(lane % side, lax.broadcasted_iota(jnp.int32, (side, LEAVES), 0)),
    )
    lane = lax.broadcasted_iota(jnp.int32, (count, LEAVES), 1)
    row = lax.broadcasted_iota(jnp.int32, (count, LEAVES), 0)
    kept = jnp.where(lane // side == row % side, spread, 0.0)
    rows = [
        jnp.sum(kept[number * side : (number + 1) * side], axis=0, keepdims=True)
        for number in range(count // side)
    ]
    blank = jnp.zeros((1, LEAVES), F32)
    lines = [
        jnp.concatenate(pair, axis=1)
        for pair in ((rows[0], blank), (rows[1], blank), (rows[2], rows[3]), (rows[4], blank))
    ]
    lines = jnp.concatenate(lines + [jnp.zeros((4, 2 * LEAVES), F32)], axis=0).astype(BF16)
    moments = moments_ref[...]
    block[...] = jnp.concatenate([moments[:, :HALF], moments[:, HALF:], lines], axis=0)
    stores = [
        pltpu.make_async_copy(block, out_ref.at[peer], out_sem.at[peer])
        for peer in range(out_ref.shape[0])
    ]
    for store in stores:
        store.start()
    for store in stores:
        store.wait()


def count_tables(parity_ref, list_ref, op_ref, counts_ref):
    leaf_list = list_ref[...]
    side = 8
    span = 2 * side + 1
    leaf = lax.broadcasted_iota(jnp.int32, leaf_list.shape, 0)
    first = leaf // side + leaf_list // span
    second = leaf % side + leaf_list % span
    codes = (
        (first // side) * BLOCKS
        + (second // side) * LEAVES
        + (first % side) * side
        + second % side
    )
    square = (SLOTS, SLOTS)
    eye = one_hot(
        lax.broadcasted_iota(jnp.int32, square, 0), lax.broadcasted_iota(jnp.int32, square, 1)
    )
    rows = op_rows(dot_rows(eye, op_ref[...].astype(F32).astype(BF16)), 0, SLOTS)
    chosen = operator_masks(rows, SLOTS)
    place = lax.broadcasted_iota(jnp.int32, (LEAVES, BLOCKS), 1)
    parity = parity_ref[0]
    for number in range(3):
        wanted = place + (number + parity * (2 - 2 * number)) * BLOCKS
        hits = jnp.concatenate(
            [one_hot(codes[:, s : s + 1], wanted) for s in range(SLOTS)], axis=0
        )
        counts_ref[number] = dot(chosen, hits).astype(BF16)


def eval_tables(rows_ref, cols_ref, left_ref, right_high_ref, right_low_ref):
    harmonics, side = rows_ref.shape
    rows = jnp.concatenate([rows_ref[...]] * 4, axis=0)
    rows = jnp.where(
        lax.broadcasted_iota(jnp.int32, rows.shape, 0) // harmonics
        == lax.broadcasted_iota(jnp.int32, rows.shape, 1) // (side // 4),
        rows,
        0.0,
    )
    high, low = halves(rows.T)
    left_ref[...] = jnp.concatenate([high, high, low, low], axis=1)
    for ref, part in zip((right_high_ref, right_low_ref), halves(cols_ref[...])):
        ref[...] = jnp.zeros_like(ref)
        for row in range(harmonics):
            ref[row * harmonics : (row + 1) * harmonics, row * side : (row + 1) * side] = part


def column_of(ref):
    side = ref.shape[0]
    leaf = lax.broadcasted_iota(jnp.int32, (LEAVES, side), 0)
    place = lax.broadcasted_iota(jnp.int32, (LEAVES, side), 1)
    spread = dot(one_hot(leaf // side, place), ref[...].astype(F32).astype(BF16))
    kept = jnp.where(leaf % side == place, spread, 0.0)
    return jnp.sum(kept, axis=1, keepdims=True).astype(jnp.int32)


def ready_kernel(
    parity_ref,
    src_ref,
    kind_ref,
    count_ref,
    density_ref,
    kinds_ref,
    list_ref,
    op_ref,
    rows_ref,
    cols_ref,
    out_ref,
    counts_ref,
    left_ref,
    right_high_ref,
    right_low_ref,
    products,
):
    near_field(src_ref, kind_ref, count_ref, density_ref, kinds_ref, out_ref, products)
    count_tables(parity_ref, list_ref, op_ref, counts_ref)
    eval_tables(rows_ref, cols_ref, left_ref, right_high_ref, right_low_ref)


def parent_kernel(own_ref, gathered_ref, shift_ref, window_ref, parents_ref):
    peers = gathered_ref.shape[0]
    flat = (peers * LEAVES, HALF)
    sources = jnp.concatenate(
        [
            gathered_ref[:, :LEAVES, :].reshape(flat),
            gathered_ref[:, LEAVES : 2 * LEAVES, :].reshape(flat),
        ],
        axis=1,
    )
    labels = []
    for peer in range(peers):
        numbers = gathered_ref[peer, 2 * LEAVES :, :].astype(F32)
        labels.append(numbers[0:1, :LEAVES] + numbers[1:2, :LEAVES] * float(PARENTS))
    labels = jnp.concatenate(labels, axis=1).astype(jnp.int32)
    positions = lax.broadcasted_iota(jnp.int32, (PARENTS, peers * LEAVES), 0)
    ordered = [
        dot(one_hot(labels, positions + octant * PARENTS), sources).astype(BF16)
        for octant in range(OCTANTS)
    ]
    total = jnp.zeros((PARENTS, COEFFS), F32)
    for octant in range(OCTANTS):
        total = total + dot(ordered[octant], shift_ref[octant])
    parents = total.astype(BF16)
    parents_ref[...] = parents
    window_ref[:PARENTS, :] = parents
    own = own_ref[0]
    for place in range(3):
        peer = lax.rem(own + place + peers - 1, peers)
        rows = slice(PARENTS + place * LEAVES, PARENTS + (place + 1) * LEAVES)
        window_ref[rows, :HALF] = gathered_ref[peer, :LEAVES, :]
        window_ref[rows, HALF:] = gathered_ref[peer, LEAVES : 2 * LEAVES, :]


def op_rows(numbers, first, slots):
    rows = [numbers[first + slot : first + slot + 1, :] for slot in range(slots)]
    return jnp.concatenate(rows, axis=1)


def operator_masks(rows, slots):
    shape = (LEAVES, slots * LEAVES)
    same = (lax.broadcasted_iota(jnp.int32, shape, 1) % LEAVES) == lax.broadcasted_iota(
        jnp.int32, shape, 0
    )
    diagonal = jnp.where(same, rows, -1.0)
    return jnp.concatenate([one_hot(diagonal, float(op)) for op in range(OPS)], axis=0)


def pick_table():
    shape = (16, COEFFS)
    row = lax.broadcasted_iota(jnp.int32, shape, 0)
    lane = lax.broadcasted_iota(jnp.int32, shape, 1)
    part, slot = lane // LEAVES, lane % PSLOTS
    value = jnp.where(part == 0, 128.0, 1.0)
    hit = (part < 2) & (row == slot) | (part == 2) & (row == slot + PSLOTS)
    return jnp.where(hit, value, 0.0).astype(BF16)


def coarse_kernel(
    parity_ref,
    parent_ref,
    gathered_ref,
    own_ref,
    counts_ref,
    leaf_ref,
    coarse_ref,
    coarse_counts_ref,
):
    leaf_ref[...] = dot(counts_ref[1], own_ref[PARENTS:, :])
    peers = gathered_ref.shape[0]
    parent_of = column_of(parent_ref)
    pick = pick_table()
    lists = []
    for peer in range(peers):
        numbers = gathered_ref[peer, 2 * LEAVES :, :].astype(F32)
        lists.append(jnp.concatenate([numbers[2:3], numbers[3:4]], axis=1))
    lists = jnp.concatenate(lists, axis=0).astype(BF16)
    owner = one_hot(parent_of // 8, lax.broadcasted_iota(jnp.int32, (LEAVES, peers), 1))
    entries = dot(owner, lists)
    lane = lax.broadcasted_iota(jnp.int32, (LEAVES, COEFFS), 1)
    entries = jnp.where((lane % LEAVES) // 8 == parent_of % 8, entries, 0.0).astype(BF16)
    by_leaf = dot_rows(entries, pick).astype(jnp.int32)
    by_slot = dot_rows(pick, entries)
    chosen = operator_masks(op_rows(by_slot, PSLOTS, PSLOTS), PSLOTS)
    column = lax.broadcasted_iota(jnp.int32, (LEAVES, PARENTS), 1)
    parity = parity_ref[0]
    for number in range(5):
        wanted = column + (number + parity * (4 - 2 * number)) * PARENTS
        hits = jnp.concatenate(
            [one_hot(by_leaf[:, s : s + 1], wanted) for s in range(PSLOTS)], axis=0
        )
        counts = dot(chosen, hits).astype(BF16)
        if number == 2:
            coarse_ref[...] = dot(counts, own_ref[:PARENTS, :])
        else:
            lanes = (number - (number > 2)) * PARENTS
            coarse_counts_ref[:, lanes : lanes + PARENTS] = counts


def final_kernel(
    octant_ref,
    counts_ref,
    leaf_ref,
    coarse_ref,
    coarse_counts_ref,
    near2_ref,
    near1_ref,
    mate_ref,
    far2_ref,
    operators_ref,
    shift_ref,
    left_ref,
    right_high_ref,
    right_low_ref,
    near_ref,
    out_ref,
    staged,
):
    leaf_sums = (
        leaf_ref[...]
        + dot(counts_ref[0], near1_ref[PARENTS:, :])
        + dot(counts_ref[2], mate_ref[PARENTS:, :])
    )
    coarse_sums = (
        coarse_ref[...]
        + dot(
            coarse_counts_ref[:, : 2 * PARENTS],
            jnp.concatenate([near2_ref[...], near1_ref[:PARENTS, :]], axis=0),
        )
        + dot(
            coarse_counts_ref[:, 2 * PARENTS :],
            jnp.concatenate([mate_ref[:PARENTS, :], far2_ref[...]], axis=0),
        )
    )

    leaf_high, leaf_low = halves(leaf_sums)
    coarse_high, coarse_low = halves(coarse_sums)
    total = jnp.zeros((4 * LEAVES, COEFFS), F32)
    for op in range(OPS):
        rows = slice(op * LEAVES, (op + 1) * LEAVES)
        stacked = jnp.concatenate(
            [leaf_high[rows], leaf_low[rows], coarse_high[rows], coarse_low[rows]], axis=0
        )
        total = total + dot(stacked, operators_ref[op])
    local = total[:LEAVES] + total[LEAVES : 2 * LEAVES]
    coarse_local = total[2 * LEAVES : 3 * LEAVES] + total[3 * LEAVES :]
    coarse_local = coarse_local.astype(BF16).astype(F32)
    octant_of = column_of(octant_ref)
    for octant in range(OCTANTS):
        chosen = jnp.where(octant_of == octant, coarse_local, 0.0).astype(BF16)
        local = local + dot_rows(chosen, shift_ref[octant])

    high, low = halves(local)
    spread = dot(jnp.concatenate([high, low], axis=0), right_high_ref[...])
    spread = spread[:LEAVES] + spread[LEAVES:] + dot(high, right_low_ref[...])
    harmonics = 16
    side = out_ref.shape[1]
    for row in range(harmonics):
        staged[pl.ds(row, LEAVES, stride=harmonics), :] = spread[:, row * side : (row + 1) * side]
    left = left_ref[...]
    for pair in range(out_ref.shape[0] // 2):
        parts = []
        for tile in (2 * pair, 2 * pair + 1):
            tile_high, tile_low = halves(staged[tile * LEAVES : (tile + 1) * LEAVES, :])
            parts.append(jnp.concatenate([tile_high, tile_low, tile_high, tile_low], axis=0))
        far = dot(left, jnp.concatenate(parts, axis=1))
        for half, tile in enumerate((2 * pair, 2 * pair + 1)):
            out_ref[tile] = (near_ref[tile] + far[:, half * side : (half + 1) * side]).astype(BF16)


VMEM = pl.BlockSpec(memory_space=pltpu.VMEM)
SMEM = pl.BlockSpec(memory_space=pltpu.SMEM)
HBM = pl.BlockSpec(memory_space=pltpu.HBM)


def ready_call(*operands):
    density, kinds = operands[4:6]
    tiles, side, _ = density.shape
    right = jax.ShapeDtypeStruct((COEFFS, 16 * side), BF16)
    return pl.pallas_call(
        ready_kernel,
        name="ready",
        out_shape=(
            jax.ShapeDtypeStruct((tiles, side, side), F32),
            jax.ShapeDtypeStruct((3, OPS * LEAVES, BLOCKS), BF16),
            jax.ShapeDtypeStruct((side, 4 * LEAVES), BF16),
            right,
            right,
        ),
        in_specs=[SMEM] * 4 + [VMEM] * 6,
        out_specs=(VMEM,) * 5,
        scratch_shapes=[pltpu.VMEM((tiles, kinds.shape[0], side, side), F32)],
        compiler_params=pltpu.CompilerParams(vmem_limit_bytes=67043328 - 4 * MIB // 2),
        cost_estimate=pl.CostEstimate(
            flops=8 * 10**9, bytes_accessed=6 * MIB, transcendentals=0
        ),
    )(*operands)


def payload_call(peers, *operands):
    return pl.pallas_call(
        payload_kernel,
        name="payload",
        out_shape=jax.ShapeDtypeStruct((peers, ROWS, HALF), BF16),
        in_specs=[HBM] * len(operands),
        out_specs=HBM,
        scratch_shapes=[pltpu.VMEM(operand.shape, operand.dtype) for operand in operands]
        + [
            pltpu.VMEM((ROWS, HALF), BF16),
            pltpu.SemaphoreType.DMA((len(operands),)),
            pltpu.SemaphoreType.DMA((peers,)),
        ],
        compiler_params=pltpu.CompilerParams(vmem_limit_bytes=67043328),
        cost_estimate=pl.CostEstimate(
            flops=10**9, bytes_accessed=MIB, transcendentals=0
        ),
    )(*operands)


def parent_call(own, gathered, shift_up):
    return pl.pallas_call(
        parent_kernel,
        name="parents",
        out_shape=(
            jax.ShapeDtypeStruct((PARENTS + BLOCKS, COEFFS), BF16),
            jax.ShapeDtypeStruct((PARENTS, COEFFS), BF16),
        ),
        in_specs=[SMEM, VMEM, VMEM],
        out_specs=(VMEM, VMEM),
        compiler_params=pltpu.CompilerParams(vmem_limit_bytes=12 * MIB),
        cost_estimate=pl.CostEstimate(
            flops=2 * 10**9, bytes_accessed=2 * MIB, transcendentals=0
        ),
    )(own, gathered, shift_up)


def coarse_call(*operands):
    rows = OPS * LEAVES
    return pl.pallas_call(
        coarse_kernel,
        name="coarse",
        out_shape=(
            jax.ShapeDtypeStruct((rows, COEFFS), F32),
            jax.ShapeDtypeStruct((rows, COEFFS), F32),
            jax.ShapeDtypeStruct((rows, 4 * PARENTS), BF16),
        ),
        in_specs=[SMEM] + [VMEM] * (len(operands) - 1),
        out_specs=(VMEM, VMEM, VMEM),
        compiler_params=pltpu.CompilerParams(vmem_limit_bytes=16 * MIB),
        cost_estimate=pl.CostEstimate(
            flops=3 * 10**9, bytes_accessed=4 * MIB, transcendentals=0
        ),
    )(*operands)


def final_call(*operands):
    near = operands[-1]
    return pl.pallas_call(
        final_kernel,
        name="final",
        out_shape=jax.ShapeDtypeStruct(near.shape, BF16),
        in_specs=[VMEM] * len(operands),
        out_specs=VMEM,
        scratch_shapes=[pltpu.VMEM((LEAVES * 16, near.shape[1]), F32)],
        compiler_params=pltpu.CompilerParams(vmem_limit_bytes=20 * MIB),
        cost_estimate=pl.CostEstimate(
            flops=4 * 10**9, bytes_accessed=8 * MIB, transcendentals=0
        ),
    )(*operands)


def routed(value, axis, to_even, to_odd):
    peers = lax.axis_size(axis)
    route = [(i, (i + (to_odd if i % 2 else to_even)) % peers) for i in range(peers)]
    return lax.ppermute(value, axis, route)


def body(
    leaf_moments,
    leaf_list,
    leaf_op,
    leaf_parent,
    leaf_octant,
    parent_list,
    parent_op,
    operators,
    shift_up,
    density,
    nearby_coulomb_kernel,
    near_src,
    near_kind,
    near_count,
    eval_rows,
    eval_cols,
):
    own = lax.axis_index("yz").astype(jnp.int32).reshape(1)
    parity = (lax.axis_index("gx") % 2).astype(jnp.int32).reshape(1)
    sent = payload_call(
        lax.axis_size("yz"),
        leaf_moments.reshape(LEAVES, COEFFS),
        leaf_parent,
        leaf_octant,
        parent_list[0],
        parent_op[0],
    )
    gathered = lax.all_to_all(sent, "yz", split_axis=0, concat_axis=0, tiled=True)

    near, counts, left, right_high, right_low = ready_call(
        parity,
        near_src,
        near_kind,
        near_count,
        density,
        nearby_coulomb_kernel,
        leaf_list.reshape(LEAVES, SLOTS),
        leaf_op.reshape(LEAVES, SLOTS),
        eval_rows.T,
        eval_cols,
    )

    window, parents = parent_call(own, gathered, shift_up)
    near1 = routed(window, "gx", -1, 1)
    mate = routed(window, "gx", 1, -1)
    near2 = routed(parents, "gx", 2, -2)
    far2 = routed(parents, "gx", -2, 2)
    leaf, coarse, coarse_counts = coarse_call(
        parity, leaf_parent, gathered, window, counts
    )
    return final_call(
        leaf_octant,
        counts,
        leaf,
        coarse,
        coarse_counts,
        near2,
        near1,
        mate,
        far2,
        operators,
        shift_up,
        left,
        right_high,
        right_low,
        near,
    )


def solution(mesh):
    in_specs = (
        P("gx", "yz", None),
        P("gx", "yz", None),
        P("gx", "yz", None),
        P("gx", "yz"),
        P("gx", "yz"),
        P("gx", "yz", None),
        P("gx", "yz", None),
        P(),
        P(),
        P(("gx", "yz"), None, None),
        P(),
        P(("gx", "yz"), None),
        P(("gx", "yz"), None),
        P(("gx", "yz")),
        P(),
        P(),
    )
    out_specs = P(("gx", "yz"), None, None)
    return jax.shard_map(body, mesh=mesh, in_specs=in_specs, out_specs=out_specs, check_vma=False)
```

```python
import functools

import jax
import jax.numpy as jnp
from jax import lax
from jax.experimental import pallas as pl
from jax.experimental.pallas import tpu as pltpu
from jax.sharding import PartitionSpec as P

BF16 = jnp.bfloat16
F32 = jnp.float32
LEAVES = 64
ROWS = 136
COEFFS = 256
HALF = 128
BLOCKS = 3 * LEAVES
PARENTS = 128
EDGE = 2 * PARENTS
OPS = 16
OCTANTS = 8
SLOTS = 16
PSLOTS = 8
MIB = 1024 * 1024
ALL_VMEM = 67043328
TABLE_LIMIT = 16 * MIB


def dot(a, b):
    return jnp.dot(a, b, preferred_element_type=F32)


def dot_rows(a, b):
    return lax.dot_general(a, b, (((1,), (1,)), ((), ())), preferred_element_type=F32)


def one_hot(labels, positions):
    return jnp.where(labels == positions, 1.0, 0.0).astype(BF16)


def halves(x):
    high = x.astype(BF16)
    return high, (x - high.astype(F32)).astype(BF16)


def near_kernel(src_ref, kind_ref, count_ref, density_ref, kinds_ref, out_ref, products):
    kinds_count, side, _ = kinds_ref.shape
    tiles = density_ref.shape[0]
    stacked = kinds_ref[...].reshape(kinds_count * side, side)

    @pl.loop(0, tiles // 2)
    def _(pair):
        both = jnp.concatenate([density_ref[2 * pair], density_ref[2 * pair + 1]], axis=1)
        made = dot(stacked, both)
        for half in range(2):
            products[2 * pair + half] = made[:, half * side : (half + 1) * side].reshape(
                kinds_count, side, side
            )

    @pl.loop(0, tiles)
    def _(tile):
        def add(slot, total):
            return total + products[src_ref[tile, slot], kind_ref[tile, slot]]

        out_ref[tile] = lax.fori_loop(
            0, count_ref[tile], add, jnp.zeros((side, side), F32)
        )


def payload_kernel(*refs):
    sources, out_ref, held, block, in_sem, out_sem = refs[:5], refs[5], refs[6:11], *refs[11:]
    fetches = [
        pltpu.make_async_copy(source, target, in_sem.at[number])
        for number, (source, target) in enumerate(zip(sources, held))
    ]
    for fetch in fetches:
        fetch.start()
    for fetch in fetches:
        fetch.wait()
    moments_ref, parent_ref, octant_ref, list_ref, op_ref = held
    coarse = list_ref[...]
    numbers = jnp.concatenate(
        [parent_ref[...], octant_ref[...], coarse >> 7, coarse & 127, op_ref[...]], axis=0
    )
    count, side = numbers.shape
    lane = lax.broadcasted_iota(jnp.int32, (side, LEAVES), 1)
    spread = dot(
        numbers.astype(F32).astype(BF16),
        one_hot(lane % side, lax.broadcasted_iota(jnp.int32, (side, LEAVES), 0)),
    )
    lane = lax.broadcasted_iota(jnp.int32, (count, LEAVES), 1)
    row = lax.broadcasted_iota(jnp.int32, (count, LEAVES), 0)
    kept = jnp.where(lane // side == row % side, spread, 0.0)
    rows = [
        jnp.sum(kept[number * side : (number + 1) * side], axis=0, keepdims=True)
        for number in range(count // side)
    ]
    blank = jnp.zeros((1, LEAVES), F32)
    lines = [
        jnp.concatenate(pair, axis=1)
        for pair in ((rows[0], blank), (rows[1], blank), (rows[2], rows[3]), (rows[4], blank))
    ]
    lines = jnp.concatenate(lines + [jnp.zeros((4, 2 * LEAVES), F32)], axis=0).astype(BF16)
    moments = moments_ref[...]
    block[...] = jnp.concatenate([moments[:, :HALF], moments[:, HALF:], lines], axis=0)
    stores = [
        pltpu.make_async_copy(block, out_ref.at[peer], out_sem.at[peer])
        for peer in range(out_ref.shape[0])
    ]
    for store in stores:
        store.start()
    for store in stores:
        store.wait()


def count_tables(parity_ref, list_ref, op_ref, counts_ref):
    leaf_list = list_ref[...]
    side = 8
    span = 2 * side + 1
    leaf = lax.broadcasted_iota(jnp.int32, leaf_list.shape, 0)
    first = leaf // side + leaf_list // span
    second = leaf % side + leaf_list % span
    codes = (
        (first // side) * BLOCKS
        + (second // side) * LEAVES
        + (first % side) * side
        + second % side
    )
    square = (SLOTS, SLOTS)
    eye = one_hot(
        lax.broadcasted_iota(jnp.int32, square, 0), lax.broadcasted_iota(jnp.int32, square, 1)
    )
    rows = op_rows(dot_rows(eye, op_ref[...].astype(F32).astype(BF16)), 0, SLOTS)
    chosen = operator_masks(rows, SLOTS)
    place = lax.broadcasted_iota(jnp.int32, (LEAVES, BLOCKS), 1)
    parity = parity_ref[0]
    for number in range(3):
        wanted = place + (number + parity * (2 - 2 * number)) * BLOCKS
        hits = jnp.concatenate(
            [one_hot(codes[:, s : s + 1], wanted) for s in range(SLOTS)], axis=0
        )
        counts_ref[number] = dot(chosen, hits).astype(BF16)


def eval_tables(rows_ref, cols_ref, left_ref, right_high_ref, right_low_ref):
    harmonics, side = rows_ref.shape
    rows = jnp.concatenate([rows_ref[...]] * 4, axis=0)
    rows = jnp.where(
        lax.broadcasted_iota(jnp.int32, rows.shape, 0) // harmonics
        == lax.broadcasted_iota(jnp.int32, rows.shape, 1) // (side // 4),
        rows,
        0.0,
    )
    high, low = halves(rows.T)
    left_ref[...] = jnp.concatenate([high, high, low, low], axis=1)
    for ref, part in zip((right_high_ref, right_low_ref), halves(cols_ref[...])):
        ref[...] = jnp.zeros_like(ref)
        for row in range(harmonics):
            ref[row * harmonics : (row + 1) * harmonics, row * side : (row + 1) * side] = part


def column_of(ref):
    side = ref.shape[0]
    leaf = lax.broadcasted_iota(jnp.int32, (LEAVES, side), 0)
    place = lax.broadcasted_iota(jnp.int32, (LEAVES, side), 1)
    spread = dot(one_hot(leaf // side, place), ref[...].astype(F32).astype(BF16))
    kept = jnp.where(leaf % side == place, spread, 0.0)
    return jnp.sum(kept, axis=1, keepdims=True).astype(jnp.int32)


def table_kernel(
    parity_ref,
    list_ref,
    op_ref,
    rows_ref,
    cols_ref,
    _,
    counts_ref,
    left_ref,
    right_high_ref,
    right_low_ref,
):
    count_tables(parity_ref, list_ref, op_ref, counts_ref)
    eval_tables(rows_ref, cols_ref, left_ref, right_high_ref, right_low_ref)


def partial_kernel(own_ref, gathered_ref, shift_ref, sums_ref):
    peers = gathered_ref.shape[0]
    flat = (peers * LEAVES, HALF)
    sources = jnp.concatenate(
        [
            gathered_ref[:, :LEAVES, :].reshape(flat),
            gathered_ref[:, LEAVES : 2 * LEAVES, :].reshape(flat),
        ],
        axis=1,
    )
    labels, lists = [], []
    for peer in range(peers):
        numbers = gathered_ref[peer, 2 * LEAVES :, :].astype(F32)
        labels.append(numbers[0:1, :LEAVES] + numbers[1:2, :LEAVES] * float(PARENTS))
        lists.append(jnp.concatenate([numbers[2:3], numbers[3:4]], axis=1))
    labels = jnp.concatenate(labels, axis=1).astype(jnp.int32)
    positions = lax.broadcasted_iota(jnp.int32, (PARENTS, peers * LEAVES), 0)
    total = jnp.zeros((PARENTS, COEFFS), F32)
    for octant in range(OCTANTS):
        chosen = one_hot(labels, positions + octant * PARENTS)
        total = total + dot(dot(chosen, sources).astype(BF16), shift_ref[octant])
    high, low = halves(total)
    sums_ref[:PARENTS, :] = high
    sums_ref[PARENTS : 2 * PARENTS, :] = low
    edge = jnp.where(own_ref[0] % peers < peers // 2, peers - 1, 0)
    rows = slice(EDGE, EDGE + LEAVES)
    sums_ref[rows, :HALF] = gathered_ref[edge, :LEAVES, :]
    sums_ref[rows, HALF:] = gathered_ref[edge, LEAVES : 2 * LEAVES, :]
    sums_ref[EDGE + LEAVES :, :] = jnp.concatenate(lists, axis=0).astype(BF16)


def parent_kernel(own_ref, gathered_ref, sums_ref, other_ref, window_ref, parents_ref):
    peers = gathered_ref.shape[0]
    total = jnp.zeros((PARENTS, COEFFS), F32)
    for ref in (sums_ref, other_ref):
        total = total + (
            ref[:PARENTS, :].astype(F32) + ref[PARENTS : 2 * PARENTS, :].astype(F32)
        )
    parents = total.astype(BF16)
    parents_ref[...] = parents
    window_ref[:PARENTS, :] = parents
    own = lax.rem(own_ref[0], peers)
    for place in range(3):
        peer = lax.rem(own + place + peers - 1, peers)
        rows = slice(PARENTS + place * LEAVES, PARENTS + (place + 1) * LEAVES)
        window_ref[rows, :HALF] = gathered_ref[peer, :LEAVES, :]
        window_ref[rows, HALF:] = gathered_ref[peer, LEAVES : 2 * LEAVES, :]

    @pl.when(own == 0)
    def _():
        window_ref[PARENTS : PARENTS + LEAVES, :] = other_ref[EDGE : EDGE + LEAVES, :]

    @pl.when(own == peers - 1)
    def _():
        window_ref[PARENTS + 2 * LEAVES :, :] = other_ref[EDGE : EDGE + LEAVES, :]


def op_rows(numbers, first, slots):
    rows = [numbers[first + slot : first + slot + 1, :] for slot in range(slots)]
    return jnp.concatenate(rows, axis=1)


def operator_masks(rows, slots):
    shape = (LEAVES, slots * LEAVES)
    same = (lax.broadcasted_iota(jnp.int32, shape, 1) % LEAVES) == lax.broadcasted_iota(
        jnp.int32, shape, 0
    )
    diagonal = jnp.where(same, rows, -1.0)
    return jnp.concatenate([one_hot(diagonal, float(op)) for op in range(OPS)], axis=0)


def pick_table():
    shape = (16, COEFFS)
    row = lax.broadcasted_iota(jnp.int32, shape, 0)
    lane = lax.broadcasted_iota(jnp.int32, shape, 1)
    part, slot = lane // LEAVES, lane % PSLOTS
    value = jnp.where(part == 0, 128.0, 1.0)
    hit = (part < 2) & (row == slot) | (part == 2) & (row == slot + PSLOTS)
    return jnp.where(hit, value, 0.0).astype(BF16)


def coarse_kernel(
    own_ref,
    parity_ref,
    parent_ref,
    sums_ref,
    other_ref,
    window_ref,
    counts_ref,
    leaf_ref,
    coarse_ref,
    coarse_counts_ref,
):
    leaf_ref[...] = dot(counts_ref[1], window_ref[PARENTS:, :])
    parent_of = column_of(parent_ref)
    pick = pick_table()
    lists = jnp.concatenate(
        [ref[EDGE + LEAVES :, :].astype(F32) for ref in (sums_ref, other_ref)], axis=0
    ).astype(BF16)
    peers = lists.shape[0]
    half = own_ref[0] // (peers // 2) * (peers // 2)
    owner = one_hot(
        (parent_of // 8 + half) % peers, lax.broadcasted_iota(jnp.int32, (LEAVES, peers), 1)
    )
    entries = dot(owner, lists)
    lane = lax.broadcasted_iota(jnp.int32, (LEAVES, COEFFS), 1)
    entries = jnp.where((lane % LEAVES) // 8 == parent_of % 8, entries, 0.0).astype(BF16)
    by_leaf = dot_rows(entries, pick).astype(jnp.int32)
    by_slot = dot_rows(pick, entries)
    chosen = operator_masks(op_rows(by_slot, PSLOTS, PSLOTS), PSLOTS)
    column = lax.broadcasted_iota(jnp.int32, (LEAVES, PARENTS), 1)
    parity = parity_ref[0]
    for number, lanes in ((0, 2), (1, 0), (2, None), (3, 1), (4, 3)):
        wanted = column + (number + parity * (4 - 2 * number)) * PARENTS
        hits = jnp.concatenate(
            [one_hot(by_leaf[:, s : s + 1], wanted) for s in range(PSLOTS)], axis=0
        )
        counts = dot(chosen, hits).astype(BF16)
        if lanes is None:
            coarse_ref[...] = dot(counts, window_ref[:PARENTS, :])
        else:
            coarse_counts_ref[:, lanes * PARENTS : (lanes + 1) * PARENTS] = counts


def operated(sums, operators_ref):
    high, low = halves(sums)
    total = jnp.zeros((2 * LEAVES, COEFFS), F32)
    for op in range(OPS):
        rows = slice(op * LEAVES, (op + 1) * LEAVES)
        total = total + dot(
            jnp.concatenate([high[rows], low[rows]], axis=0), operators_ref[op]
        )
    return total[:LEAVES] + total[LEAVES:]


def leaf_kernel(
    counts_ref,
    leaf_ref,
    coarse_ref,
    coarse_counts_ref,
    near1_ref,
    mate_ref,
    operators_ref,
    local_ref,
    partial_ref,
):
    leaf_sums = (
        leaf_ref[...]
        + dot(counts_ref[0], near1_ref[PARENTS:, :])
        + dot(counts_ref[2], mate_ref[PARENTS:, :])
    )
    partial_ref[...] = coarse_ref[...] + dot(
        coarse_counts_ref[:, : 2 * PARENTS],
        jnp.concatenate([near1_ref[:PARENTS, :], mate_ref[:PARENTS, :]], axis=0),
    )
    local_ref[...] = operated(leaf_sums, operators_ref)


def final_kernel(
    octant_ref,
    local_ref,
    partial_ref,
    coarse_counts_ref,
    near2_ref,
    far2_ref,
    operators_ref,
    shift_ref,
    left_ref,
    right_high_ref,
    right_low_ref,
    near_ref,
    out_ref,
    staged,
):
    coarse_sums = partial_ref[...] + dot(
        coarse_counts_ref[:, 2 * PARENTS :],
        jnp.concatenate([near2_ref[...], far2_ref[...]], axis=0),
    )
    coarse_local = operated(coarse_sums, operators_ref).astype(BF16).astype(F32)
    octant_of = column_of(octant_ref)
    local = local_ref[...]
    for octant in range(OCTANTS):
        chosen = jnp.where(octant_of == octant, coarse_local, 0.0).astype(BF16)
        local = local + dot_rows(chosen, shift_ref[octant])

    high, low = halves(local)
    spread = dot(jnp.concatenate([high, low], axis=0), right_high_ref[...])
    spread = spread[:LEAVES] + spread[LEAVES:] + dot(high, right_low_ref[...])
    harmonics = 16
    side = out_ref.shape[1]
    for row in range(harmonics):
        staged[pl.ds(row, LEAVES, stride=harmonics), :] = spread[:, row * side : (row + 1) * side]
    left = left_ref[...]
    for pair in range(out_ref.shape[0] // 2):
        parts = []
        for tile in (2 * pair, 2 * pair + 1):
            tile_high, tile_low = halves(staged[tile * LEAVES : (tile + 1) * LEAVES, :])
            parts.append(jnp.concatenate([tile_high, tile_low, tile_high, tile_low], axis=0))
        far = dot(left, jnp.concatenate(parts, axis=1))
        for half, tile in enumerate((2 * pair, 2 * pair + 1)):
            out_ref[tile] = (near_ref[tile] + far[:, half * side : (half + 1) * side]).astype(BF16)


VMEM = pl.BlockSpec(memory_space=pltpu.VMEM)
SMEM = pl.BlockSpec(memory_space=pltpu.SMEM)
HBM = pl.BlockSpec(memory_space=pltpu.HBM)


def call(kernel, name, outs, specs, operands, limit, flops, scratch=()):
    out_shape = tuple(jax.ShapeDtypeStruct(shape, kind) for shape, kind in outs)
    moved = sum(operand.size * operand.dtype.itemsize for operand in operands)
    return pl.pallas_call(
        kernel,
        name=name,
        out_shape=out_shape,
        in_specs=specs + [VMEM] * (len(operands) - len(specs)),
        out_specs=(VMEM,) * len(outs),
        scratch_shapes=list(scratch),
        compiler_params=pltpu.CompilerParams(vmem_limit_bytes=limit),
        cost_estimate=pl.CostEstimate(flops=flops, bytes_accessed=moved, transcendentals=0),
    )(*operands)


def payload_call(peers, *operands):
    return pl.pallas_call(
        payload_kernel,
        name="payload",
        out_shape=jax.ShapeDtypeStruct((peers, ROWS, HALF), BF16),
        in_specs=[HBM] * len(operands),
        out_specs=HBM,
        scratch_shapes=[pltpu.VMEM(operand.shape, operand.dtype) for operand in operands]
        + [
            pltpu.VMEM((ROWS, HALF), BF16),
            pltpu.SemaphoreType.DMA((len(operands),)),
            pltpu.SemaphoreType.DMA((peers,)),
        ],
        compiler_params=pltpu.CompilerParams(vmem_limit_bytes=ALL_VMEM),
        cost_estimate=pl.CostEstimate(
            flops=10**9, bytes_accessed=MIB, transcendentals=0
        ),
    )(*operands)


def routed(value, axis, to_even, to_odd):
    peers = lax.axis_size(axis)
    route = [(i, (i + (to_odd if i % 2 else to_even)) % peers) for i in range(peers)]
    return lax.ppermute(value, axis, route)


def body(
    leaf_moments,
    leaf_list,
    leaf_op,
    leaf_parent,
    leaf_octant,
    parent_list,
    parent_op,
    operators,
    shift_up,
    density,
    nearby_coulomb_kernel,
    near_src,
    near_kind,
    near_count,
    eval_rows,
    eval_cols,
):
    own = lax.axis_index("yz").astype(jnp.int32).reshape(1)
    parity = (lax.axis_index("gx") % 2).astype(jnp.int32).reshape(1)
    column = lax.axis_size("yz")
    half = column // 2
    sent = payload_call(
        half,
        leaf_moments.reshape(LEAVES, COEFFS),
        leaf_parent,
        leaf_octant,
        parent_list[0],
        parent_op[0],
    )
    gathered = lax.all_to_all(
        sent,
        "yz",
        split_axis=0,
        concat_axis=0,
        tiled=True,
        axis_index_groups=[list(range(half)), list(range(half, column))],
    )

    tiles, side, _ = density.shape
    kinds = nearby_coulomb_kernel.shape[0]
    (near,) = call(
        near_kernel,
        "near",
        [((tiles, side, side), F32)],
        [SMEM] * 3,
        (near_src, near_kind, near_count, density, nearby_coulomb_kernel),
        ALL_VMEM - 2 * MIB,
        4 * 10**9,
        [pltpu.VMEM((tiles, kinds, side, side), F32)],
    )
    (sums,) = call(
        partial_kernel,
        "partial",
        [((EDGE + LEAVES + 8, COEFFS), BF16)],
        [SMEM],
        (own, gathered, shift_up),
        12 * MIB,
        10**9,
    )
    other = lax.ppermute(sums, "yz", [(i, (i + half) % column) for i in range(column)])
    counts, left, right_high, right_low = call(
        table_kernel,
        "table",
        [
            ((3, OPS * LEAVES, BLOCKS), BF16),
            ((side, 4 * LEAVES), BF16),
            ((COEFFS, 16 * side), BF16),
            ((COEFFS, 16 * side), BF16),
        ],
        [SMEM] + [VMEM] * 4 + [pl.BlockSpec(memory_space=pl.ANY)],
        (
            parity,
            leaf_list.reshape(LEAVES, SLOTS),
            leaf_op.reshape(LEAVES, SLOTS),
            eval_rows.T,
            eval_cols,
            sums,
        ),
        TABLE_LIMIT,
        4 * 10**9,
    )

    window, parents = call(
        parent_kernel,
        "parents",
        [((PARENTS + BLOCKS, COEFFS), BF16), ((PARENTS, COEFFS), BF16)],
        [SMEM],
        (own, gathered, sums, other),
        8 * MIB,
        10**8,
    )
    near1 = routed(window, "gx", -1, 1)
    mate = routed(window, "gx", 1, -1)
    near2 = routed(parents, "gx", 2, -2)
    far2 = routed(parents, "gx", -2, 2)
    rows = OPS * LEAVES
    leaf, coarse, coarse_counts = call(
        coarse_kernel,
        "coarse",
        [((rows, COEFFS), F32), ((rows, COEFFS), F32), ((rows, 4 * PARENTS), BF16)],
        [SMEM] * 2,
        (own, parity, leaf_parent, sums, other, window, counts),
        16 * MIB,
        3 * 10**9,
    )
    local, partial = call(
        leaf_kernel,
        "leaf",
        [((LEAVES, COEFFS), F32), ((rows, COEFFS), F32)],
        [],
        (counts, leaf, coarse, coarse_counts, near1, mate, operators),
        16 * MIB,
        2 * 10**9,
    )
    (out,) = call(
        final_kernel,
        "final",
        [((tiles, side, side), BF16)],
        [],
        (
            leaf_octant,
            local,
            partial,
            coarse_counts,
            near2,
            far2,
            operators,
            shift_up,
            left,
            right_high,
            right_low,
            near,
        ),
        20 * MIB,
        3 * 10**9,
        [pltpu.VMEM((LEAVES * 16, side), F32)],
    )
    return out


def solution(mesh):
    in_specs = (
        P("gx", "yz", None),
        P("gx", "yz", None),
        P("gx", "yz", None),
        P("gx", "yz"),
        P("gx", "yz"),
        P("gx", "yz", None),
        P("gx", "yz", None),
        P(),
        P(),
        P(("gx", "yz"), None, None),
        P(),
        P(("gx", "yz"), None),
        P(("gx", "yz"), None),
        P(("gx", "yz")),
        P(),
        P(),
    )
    out_specs = P(("gx", "yz"), None, None)
    return jax.shard_map(body, mesh=mesh, in_specs=in_specs, out_specs=out_specs, check_vma=False)
```

```python
import jax
import jax.numpy as jnp
from jax import lax
from jax.experimental import pallas as pl
from jax.experimental.pallas import tpu as pltpu
from jax.sharding import PartitionSpec as P

BF16 = jnp.bfloat16
F32 = jnp.float32
LEAVES = 64
ROWS = 136
COEFFS = 256
HALF = 128
BLOCKS = 3 * LEAVES
PARENTS = 128
OPS = 16
OCTANTS = 8
SLOTS = 16
PSLOTS = 8
MIB = 1024 * 1024


def dot(a, b):
    return jnp.dot(a, b, preferred_element_type=F32)


def dot_rows(a, b):
    return lax.dot_general(a, b, (((1,), (1,)), ((), ())), preferred_element_type=F32)


def one_hot(labels, positions):
    return jnp.where(labels == positions, 1.0, 0.0).astype(BF16)


def halves(x):
    high = x.astype(BF16)
    return high, (x - high.astype(F32)).astype(BF16)


def near_field(src_ref, kind_ref, count_ref, density_ref, kinds_ref, out_ref, products):
    kinds_count, side, _ = kinds_ref.shape
    tiles = density_ref.shape[0]
    stacked = kinds_ref[...].reshape(kinds_count * side, side)

    @pl.loop(0, tiles // 2)
    def _(pair):
        both = jnp.concatenate([density_ref[2 * pair], density_ref[2 * pair + 1]], axis=1)
        made = dot(stacked, both)
        for half in range(2):
            products[2 * pair + half] = made[:, half * side : (half + 1) * side].reshape(
                kinds_count, side, side
            )

    @pl.loop(0, tiles)
    def _(tile):
        def add(slot, total):
            return total + products[src_ref[tile, slot], kind_ref[tile, slot]]

        out_ref[tile] = lax.fori_loop(
            0, count_ref[tile], add, jnp.zeros((side, side), F32)
        )


def payload_kernel(*refs):
    sources, out_ref, held, block, in_sem, out_sem = refs[:5], refs[5], refs[6:11], *refs[11:]
    fetches = [
        pltpu.make_async_copy(source, target, in_sem.at[number])
        for number, (source, target) in enumerate(zip(sources, held))
    ]
    for fetch in fetches:
        fetch.start()
    fetches[0].wait()
    moments_ref, parent_ref, octant_ref, list_ref, op_ref = held
    block[:LEAVES, :] = moments_ref[:, :HALF]
    block[LEAVES : 2 * LEAVES, :] = moments_ref[:, HALF:]
    peers = out_ref.shape[0]
    stores = []
    for part, rows in enumerate((slice(0, 2 * LEAVES), slice(2 * LEAVES, ROWS))):
        stores.append(
            [
                pltpu.make_async_copy(
                    block.at[rows], out_ref.at[peer, rows], out_sem.at[part, peer]
                )
                for peer in range(peers)
            ]
        )
    for store in stores[0]:
        store.start()
    for fetch in fetches[1:]:
        fetch.wait()
    coarse = list_ref[...]
    numbers = jnp.concatenate(
        [parent_ref[...], octant_ref[...], coarse >> 7, coarse & 127, op_ref[...]], axis=0
    )
    count, side = numbers.shape
    lane = lax.broadcasted_iota(jnp.int32, (side, LEAVES), 1)
    spread = dot(
        numbers.astype(F32).astype(BF16),
        one_hot(lane % side, lax.broadcasted_iota(jnp.int32, (side, LEAVES), 0)),
    )
    lane = lax.broadcasted_iota(jnp.int32, (count, LEAVES), 1)
    row = lax.broadcasted_iota(jnp.int32, (count, LEAVES), 0)
    kept = jnp.where(lane // side == row % side, spread, 0.0)
    rows = [
        jnp.sum(kept[number * side : (number + 1) * side], axis=0, keepdims=True)
        for number in range(count // side)
    ]
    blank = jnp.zeros((1, LEAVES), F32)
    lines = [
        jnp.concatenate(pair, axis=1)
        for pair in ((rows[0], blank), (rows[1], blank), (rows[2], rows[3]), (rows[4], blank))
    ]
    lines = jnp.concatenate(lines + [jnp.zeros((4, 2 * LEAVES), F32)], axis=0).astype(BF16)
    block[2 * LEAVES :, :] = lines
    for store in stores[1]:
        store.start()
    for store in stores[0] + stores[1]:
        store.wait()


def count_tables(parity_ref, list_ref, op_ref, counts_ref):
    leaf_list = list_ref[...]
    side = 8
    span = 2 * side + 1
    leaf = lax.broadcasted_iota(jnp.int32, leaf_list.shape, 0)
    first = leaf // side + leaf_list // span
    second = leaf % side + leaf_list % span
    codes = (
        (first // side) * BLOCKS
        + (second // side) * LEAVES
        + (first % side) * side
        + second % side
    )
    square = (SLOTS, SLOTS)
    eye = one_hot(
        lax.broadcasted_iota(jnp.int32, square, 0), lax.broadcasted_iota(jnp.int32, square, 1)
    )
    rows = op_rows(dot_rows(eye, op_ref[...].astype(F32).astype(BF16)), 0, SLOTS)
    chosen = operator_masks(rows, SLOTS)
    place = lax.broadcasted_iota(jnp.int32, (LEAVES, BLOCKS), 1)
    parity = parity_ref[0]
    for number in range(3):
        wanted = place + (number + parity * (2 - 2 * number)) * BLOCKS
        hits = jnp.concatenate(
            [one_hot(codes[:, s : s + 1], wanted) for s in range(SLOTS)], axis=0
        )
        counts_ref[number] = dot(chosen, hits).astype(BF16)


def eval_tables(rows_ref, cols_ref, left_ref, right_high_ref, right_low_ref):
    harmonics, side = rows_ref.shape
    rows = jnp.concatenate([rows_ref[...]] * 4, axis=0)
    rows = jnp.where(
        lax.broadcasted_iota(jnp.int32, rows.shape, 0) // harmonics
        == lax.broadcasted_iota(jnp.int32, rows.shape, 1) // (side // 4),
        rows,
        0.0,
    )
    high, low = halves(rows.T)
    left_ref[...] = jnp.concatenate([high, high, low, low], axis=1)
    for ref, part in zip((right_high_ref, right_low_ref), halves(cols_ref[...])):
        ref[...] = jnp.zeros_like(ref)
        for row in range(harmonics):
            ref[row * harmonics : (row + 1) * harmonics, row * side : (row + 1) * side] = part


def column_of(ref):
    side = ref.shape[0]
    leaf = lax.broadcasted_iota(jnp.int32, (LEAVES, side), 0)
    place = lax.broadcasted_iota(jnp.int32, (LEAVES, side), 1)
    spread = dot(one_hot(leaf // side, place), ref[...].astype(F32).astype(BF16))
    kept = jnp.where(leaf % side == place, spread, 0.0)
    return jnp.sum(kept, axis=1, keepdims=True).astype(jnp.int32)


def ready_kernel(
    parity_ref,
    src_ref,
    kind_ref,
    count_ref,
    density_ref,
    kinds_ref,
    list_ref,
    op_ref,
    rows_ref,
    cols_ref,
    out_ref,
    counts_ref,
    left_ref,
    right_high_ref,
    right_low_ref,
    products,
):
    near_field(src_ref, kind_ref, count_ref, density_ref, kinds_ref, out_ref, products)
    count_tables(parity_ref, list_ref, op_ref, counts_ref)
    eval_tables(rows_ref, cols_ref, left_ref, right_high_ref, right_low_ref)


def parent_kernel(own_ref, gathered_ref, shift_ref, window_ref, parents_ref):
    peers = gathered_ref.shape[0]
    flat = (peers * LEAVES, HALF)
    sources = jnp.concatenate(
        [
            gathered_ref[:, :LEAVES, :].reshape(flat),
            gathered_ref[:, LEAVES : 2 * LEAVES, :].reshape(flat),
        ],
        axis=1,
    )
    labels = []
    for peer in range(peers):
        numbers = gathered_ref[peer, 2 * LEAVES :, :].astype(F32)
        labels.append(numbers[0:1, :LEAVES] + numbers[1:2, :LEAVES] * float(PARENTS))
    labels = jnp.concatenate(labels, axis=1).astype(jnp.int32)
    positions = lax.broadcasted_iota(jnp.int32, (PARENTS, peers * LEAVES), 0)
    ordered = [
        dot(one_hot(labels, positions + octant * PARENTS), sources).astype(BF16)
        for octant in range(OCTANTS)
    ]
    total = jnp.zeros((PARENTS, COEFFS), F32)
    for octant in range(OCTANTS):
        total = total + dot(ordered[octant], shift_ref[octant])
    parents = total.astype(BF16)
    parents_ref[...] = parents
    window_ref[:PARENTS, :] = parents
    own = own_ref[0]
    for place in range(3):
        peer = lax.rem(own + place + peers - 1, peers)
        rows = slice(PARENTS + place * LEAVES, PARENTS + (place + 1) * LEAVES)
        window_ref[rows, :HALF] = gathered_ref[peer, :LEAVES, :]
        window_ref[rows, HALF:] = gathered_ref[peer, LEAVES : 2 * LEAVES, :]


def op_rows(numbers, first, slots):
    rows = [numbers[first + slot : first + slot + 1, :] for slot in range(slots)]
    return jnp.concatenate(rows, axis=1)


def operator_masks(rows, slots):
    shape = (LEAVES, slots * LEAVES)
    same = (lax.broadcasted_iota(jnp.int32, shape, 1) % LEAVES) == lax.broadcasted_iota(
        jnp.int32, shape, 0
    )
    diagonal = jnp.where(same, rows, -1.0)
    return jnp.concatenate([one_hot(diagonal, float(op)) for op in range(OPS)], axis=0)


def pick_table():
    shape = (16, COEFFS)
    row = lax.broadcasted_iota(jnp.int32, shape, 0)
    lane = lax.broadcasted_iota(jnp.int32, shape, 1)
    part, slot = lane // LEAVES, lane % PSLOTS
    value = jnp.where(part == 0, 128.0, 1.0)
    hit = (part < 2) & (row == slot) | (part == 2) & (row == slot + PSLOTS)
    return jnp.where(hit, value, 0.0).astype(BF16)


def coarse_kernel(
    parity_ref,
    parent_ref,
    gathered_ref,
    own_ref,
    counts_ref,
    leaf_ref,
    coarse_ref,
    coarse_counts_ref,
):
    leaf_ref[...] = dot(counts_ref[1], own_ref[PARENTS:, :])
    peers = gathered_ref.shape[0]
    parent_of = column_of(parent_ref)
    pick = pick_table()
    lists = []
    for peer in range(peers):
        numbers = gathered_ref[peer, 2 * LEAVES :, :].astype(F32)
        lists.append(jnp.concatenate([numbers[2:3], numbers[3:4]], axis=1))
    lists = jnp.concatenate(lists, axis=0).astype(BF16)
    owner = one_hot(parent_of // 8, lax.broadcasted_iota(jnp.int32, (LEAVES, peers), 1))
    entries = dot(owner, lists)
    lane = lax.broadcasted_iota(jnp.int32, (LEAVES, COEFFS), 1)
    entries = jnp.where((lane % LEAVES) // 8 == parent_of % 8, entries, 0.0).astype(BF16)
    by_leaf = dot_rows(entries, pick).astype(jnp.int32)
    by_slot = dot_rows(pick, entries)
    chosen = operator_masks(op_rows(by_slot, PSLOTS, PSLOTS), PSLOTS)
    column = lax.broadcasted_iota(jnp.int32, (LEAVES, PARENTS), 1)
    parity = parity_ref[0]
    for number in range(5):
        wanted = column + (number + parity * (4 - 2 * number)) * PARENTS
        hits = jnp.concatenate(
            [one_hot(by_leaf[:, s : s + 1], wanted) for s in range(PSLOTS)], axis=0
        )
        counts = dot(chosen, hits).astype(BF16)
        if number == 2:
            coarse_ref[...] = dot(counts, own_ref[:PARENTS, :])
        else:
            lanes = (number - (number > 2)) * PARENTS
            coarse_counts_ref[:, lanes : lanes + PARENTS] = counts


def final_kernel(
    octant_ref,
    counts_ref,
    leaf_ref,
    coarse_ref,
    coarse_counts_ref,
    near2_ref,
    near1_ref,
    mate_ref,
    far2_ref,
    operators_ref,
    shift_ref,
    left_ref,
    right_high_ref,
    right_low_ref,
    near_ref,
    out_ref,
    staged,
):
    leaf_sums = (
        leaf_ref[...]
        + dot(counts_ref[0], near1_ref[PARENTS:, :])
        + dot(counts_ref[2], mate_ref[PARENTS:, :])
    )
    coarse_sums = (
        coarse_ref[...]
        + dot(
            coarse_counts_ref[:, : 2 * PARENTS],
            jnp.concatenate([near2_ref[...], near1_ref[:PARENTS, :]], axis=0),
        )
        + dot(
            coarse_counts_ref[:, 2 * PARENTS :],
            jnp.concatenate([mate_ref[:PARENTS, :], far2_ref[...]], axis=0),
        )
    )

    leaf_high, leaf_low = halves(leaf_sums)
    coarse_high, coarse_low = halves(coarse_sums)
    total = jnp.zeros((4 * LEAVES, COEFFS), F32)
    for op in range(OPS):
        rows = slice(op * LEAVES, (op + 1) * LEAVES)
        stacked = jnp.concatenate(
            [leaf_high[rows], leaf_low[rows], coarse_high[rows], coarse_low[rows]], axis=0
        )
        total = total + dot(stacked, operators_ref[op])
    local = total[:LEAVES] + total[LEAVES : 2 * LEAVES]
    coarse_local = total[2 * LEAVES : 3 * LEAVES] + total[3 * LEAVES :]
    coarse_local = coarse_local.astype(BF16).astype(F32)
    octant_of = column_of(octant_ref)
    for octant in range(OCTANTS):
        chosen = jnp.where(octant_of == octant, coarse_local, 0.0).astype(BF16)
        local = local + dot_rows(chosen, shift_ref[octant])

    high, low = halves(local)
    spread = dot(jnp.concatenate([high, low], axis=0), right_high_ref[...])
    spread = spread[:LEAVES] + spread[LEAVES:] + dot(high, right_low_ref[...])
    harmonics = 16
    side = out_ref.shape[1]
    for row in range(harmonics):
        staged[pl.ds(row, LEAVES, stride=harmonics), :] = spread[:, row * side : (row + 1) * side]
    left = left_ref[...]
    for pair in range(out_ref.shape[0] // 2):
        parts = []
        for tile in (2 * pair, 2 * pair + 1):
            tile_high, tile_low = halves(staged[tile * LEAVES : (tile + 1) * LEAVES, :])
            parts.append(jnp.concatenate([tile_high, tile_low, tile_high, tile_low], axis=0))
        far = dot(left, jnp.concatenate(parts, axis=1))
        for half, tile in enumerate((2 * pair, 2 * pair + 1)):
            out_ref[tile] = (near_ref[tile] + far[:, half * side : (half + 1) * side]).astype(BF16)


VMEM = pl.BlockSpec(memory_space=pltpu.VMEM)
SMEM = pl.BlockSpec(memory_space=pltpu.SMEM)
HBM = pl.BlockSpec(memory_space=pltpu.HBM)


def ready_call(*operands):
    density, kinds = operands[4:6]
    tiles, side, _ = density.shape
    right = jax.ShapeDtypeStruct((COEFFS, 16 * side), BF16)
    return pl.pallas_call(
        ready_kernel,
        name="ready",
        out_shape=(
            jax.ShapeDtypeStruct((tiles, side, side), F32),
            jax.ShapeDtypeStruct((3, OPS * LEAVES, BLOCKS), BF16),
            jax.ShapeDtypeStruct((side, 4 * LEAVES), BF16),
            right,
            right,
        ),
        in_specs=[SMEM] * 4 + [VMEM] * 6,
        out_specs=(VMEM,) * 5,
        scratch_shapes=[pltpu.VMEM((tiles, kinds.shape[0], side, side), F32)],
        compiler_params=pltpu.CompilerParams(vmem_limit_bytes=67043328 - 4 * MIB // 2),
        cost_estimate=pl.CostEstimate(
            flops=8 * 10**9, bytes_accessed=6 * MIB, transcendentals=0
        ),
    )(*operands)


def payload_call(peers, *operands):
    return pl.pallas_call(
        payload_kernel,
        name="payload",
        out_shape=jax.ShapeDtypeStruct((peers, ROWS, HALF), BF16),
        in_specs=[HBM] * len(operands),
        out_specs=HBM,
        scratch_shapes=[pltpu.VMEM(operand.shape, operand.dtype) for operand in operands]
        + [
            pltpu.VMEM((ROWS, HALF), BF16),
            pltpu.SemaphoreType.DMA((len(operands),)),
            pltpu.SemaphoreType.DMA((2, peers)),
        ],
        compiler_params=pltpu.CompilerParams(vmem_limit_bytes=67043328),
        cost_estimate=pl.CostEstimate(
            flops=10**9, bytes_accessed=MIB, transcendentals=0
        ),
    )(*operands)


def parent_call(own, gathered, shift_up):
    return pl.pallas_call(
        parent_kernel,
        name="parents",
        out_shape=(
            jax.ShapeDtypeStruct((PARENTS + BLOCKS, COEFFS), BF16),
            jax.ShapeDtypeStruct((PARENTS, COEFFS), BF16),
        ),
        in_specs=[SMEM, VMEM, VMEM],
        out_specs=(VMEM, VMEM),
        compiler_params=pltpu.CompilerParams(vmem_limit_bytes=12 * MIB),
        cost_estimate=pl.CostEstimate(
            flops=2 * 10**9, bytes_accessed=2 * MIB, transcendentals=0
        ),
    )(own, gathered, shift_up)


def coarse_call(*operands):
    rows = OPS * LEAVES
    return pl.pallas_call(
        coarse_kernel,
        name="coarse",
        out_shape=(
            jax.ShapeDtypeStruct((rows, COEFFS), F32),
            jax.ShapeDtypeStruct((rows, COEFFS), F32),
            jax.ShapeDtypeStruct((rows, 4 * PARENTS), BF16),
        ),
        in_specs=[SMEM] + [VMEM] * (len(operands) - 1),
        out_specs=(VMEM, VMEM, VMEM),
        compiler_params=pltpu.CompilerParams(vmem_limit_bytes=16 * MIB),
        cost_estimate=pl.CostEstimate(
            flops=3 * 10**9, bytes_accessed=4 * MIB, transcendentals=0
        ),
    )(*operands)


def final_call(*operands):
    near = operands[-1]
    return pl.pallas_call(
        final_kernel,
        name="final",
        out_shape=jax.ShapeDtypeStruct(near.shape, BF16),
        in_specs=[VMEM] * len(operands),
        out_specs=VMEM,
        scratch_shapes=[pltpu.VMEM((LEAVES * 16, near.shape[1]), F32)],
        compiler_params=pltpu.CompilerParams(vmem_limit_bytes=20 * MIB),
        cost_estimate=pl.CostEstimate(
            flops=4 * 10**9, bytes_accessed=8 * MIB, transcendentals=0
        ),
    )(*operands)


def routed(value, axis, to_even, to_odd):
    peers = lax.axis_size(axis)
    route = [(i, (i + (to_odd if i % 2 else to_even)) % peers) for i in range(peers)]
    return lax.ppermute(value, axis, route)


def body(
    leaf_moments,
    leaf_list,
    leaf_op,
    leaf_parent,
    leaf_octant,
    parent_list,
    parent_op,
    operators,
    shift_up,
    density,
    nearby_coulomb_kernel,
    near_src,
    near_kind,
    near_count,
    eval_rows,
    eval_cols,
):
    own = lax.axis_index("yz").astype(jnp.int32).reshape(1)
    parity = (lax.axis_index("gx") % 2).astype(jnp.int32).reshape(1)
    sent = payload_call(
        lax.axis_size("yz"),
        leaf_moments.reshape(LEAVES, COEFFS),
        leaf_parent,
        leaf_octant,
        parent_list[0],
        parent_op[0],
    )
    gathered = lax.all_to_all(sent, "yz", split_axis=0, concat_axis=0, tiled=True)

    near, counts, left, right_high, right_low = ready_call(
        parity,
        near_src,
        near_kind,
        near_count,
        density,
        nearby_coulomb_kernel,
        leaf_list.reshape(LEAVES, SLOTS),
        leaf_op.reshape(LEAVES, SLOTS),
        eval_rows.T,
        eval_cols,
    )

    window, parents = parent_call(own, gathered, shift_up)
    near2 = routed(parents, "gx", 2, -2)
    far2 = routed(parents, "gx", -2, 2)
    near1 = routed(window, "gx", -1, 1)
    mate = routed(window, "gx", 1, -1)
    leaf, coarse, coarse_counts = coarse_call(
        parity, leaf_parent, gathered, window, counts
    )
    return final_call(
        leaf_octant,
        counts,
        leaf,
        coarse,
        coarse_counts,
        near2,
        near1,
        mate,
        far2,
        operators,
        shift_up,
        left,
        right_high,
        right_low,
        near,
    )


def solution(mesh):
    in_specs = (
        P("gx", "yz", None),
        P("gx", "yz", None),
        P("gx", "yz", None),
        P("gx", "yz"),
        P("gx", "yz"),
        P("gx", "yz", None),
        P("gx", "yz", None),
        P(),
        P(),
        P(("gx", "yz"), None, None),
        P(),
        P(("gx", "yz"), None),
        P(("gx", "yz"), None),
        P(("gx", "yz")),
        P(),
        P(),
    )
    out_specs = P(("gx", "yz"), None, None)
    return jax.shard_map(body, mesh=mesh, in_specs=in_specs, out_specs=out_specs, check_vma=False)
```

```python
import jax
import jax.numpy as jnp
from jax import lax
from jax.experimental import pallas as pl
from jax.experimental.pallas import tpu as pltpu
from jax.sharding import PartitionSpec as P

BF16 = jnp.bfloat16
F32 = jnp.float32
LEAVES = 64
ROWS = 136
COEFFS = 256
HALF = 128
BLOCKS = 3 * LEAVES
PARENTS = 128
OPS = 16
OCTANTS = 8
SLOTS = 16
PSLOTS = 8
MIB = 1024 * 1024


def dot(a, b):
    return jnp.dot(a, b, preferred_element_type=F32)


def dot_rows(a, b):
    return lax.dot_general(a, b, (((1,), (1,)), ((), ())), preferred_element_type=F32)


def one_hot(labels, positions):
    return jnp.where(labels == positions, 1.0, 0.0).astype(BF16)


def halves(x):
    high = x.astype(BF16)
    return high, (x - high.astype(F32)).astype(BF16)


def near_field(src_ref, kind_ref, count_ref, density_ref, kinds_ref, out_ref, products):
    kinds_count, side, _ = kinds_ref.shape
    tiles = density_ref.shape[0]
    stacked = kinds_ref[...].reshape(kinds_count * side, side)

    @pl.loop(0, tiles // 2)
    def _(pair):
        both = jnp.concatenate([density_ref[2 * pair], density_ref[2 * pair + 1]], axis=1)
        made = dot(stacked, both)
        for half in range(2):
            products[2 * pair + half] = made[:, half * side : (half + 1) * side].reshape(
                kinds_count, side, side
            )

    @pl.loop(0, tiles)
    def _(tile):
        def add(slot, total):
            return total + products[src_ref[tile, slot], kind_ref[tile, slot]]

        out_ref[tile] = lax.fori_loop(
            0, count_ref[tile], add, jnp.zeros((side, side), F32)
        )


def payload_kernel(*refs):
    sources, out_ref, held, block, in_sem, out_sem = refs[:5], refs[5], refs[6:11], *refs[11:]
    fetches = [
        pltpu.make_async_copy(source, target, in_sem.at[number])
        for number, (source, target) in enumerate(zip(sources, held))
    ]
    for fetch in fetches:
        fetch.start()
    fetches[0].wait()
    moments_ref, parent_ref, octant_ref, list_ref, op_ref = held
    block[:LEAVES, :] = moments_ref[:, :HALF]
    block[LEAVES : 2 * LEAVES, :] = moments_ref[:, HALF:]
    peers = out_ref.shape[0]
    stores = []
    for part, rows in enumerate((slice(0, 2 * LEAVES), slice(2 * LEAVES, ROWS))):
        stores.append(
            [
                pltpu.make_async_copy(
                    block.at[rows], out_ref.at[peer, rows], out_sem.at[part, peer]
                )
                for peer in range(peers)
            ]
        )
    for store in stores[0]:
        store.start()
    for fetch in fetches[1:]:
        fetch.wait()
    coarse = list_ref[...]
    numbers = jnp.concatenate(
        [parent_ref[...], octant_ref[...], coarse >> 7, coarse & 127, op_ref[...]], axis=0
    )
    count, side = numbers.shape
    lane = lax.broadcasted_iota(jnp.int32, (side, LEAVES), 1)
    spread = dot(
        numbers.astype(F32).astype(BF16),
        one_hot(lane % side, lax.broadcasted_iota(jnp.int32, (side, LEAVES), 0)),
    )
    lane = lax.broadcasted_iota(jnp.int32, (count, LEAVES), 1)
    row = lax.broadcasted_iota(jnp.int32, (count, LEAVES), 0)
    kept = jnp.where(lane // side == row % side, spread, 0.0)
    rows = [
        jnp.sum(kept[number * side : (number + 1) * side], axis=0, keepdims=True)
        for number in range(count // side)
    ]
    blank = jnp.zeros((1, LEAVES), F32)
    lines = [
        jnp.concatenate(pair, axis=1)
        for pair in ((rows[0], blank), (rows[1], blank), (rows[2], rows[3]), (rows[4], blank))
    ]
    lines = jnp.concatenate(lines + [jnp.zeros((4, 2 * LEAVES), F32)], axis=0).astype(BF16)
    block[2 * LEAVES :, :] = lines
    for store in stores[1]:
        store.start()
    for store in stores[0] + stores[1]:
        store.wait()


def count_tables(parity_ref, list_ref, op_ref, counts_ref):
    leaf_list = list_ref[...]
    side = 8
    span = 2 * side + 1
    leaf = lax.broadcasted_iota(jnp.int32, leaf_list.shape, 0)
    first = leaf // side + leaf_list // span
    second = leaf % side + leaf_list % span
    codes = (
        (first // side) * BLOCKS
        + (second // side) * LEAVES
        + (first % side) * side
        + second % side
    )
    square = (SLOTS, SLOTS)
    eye = one_hot(
        lax.broadcasted_iota(jnp.int32, square, 0), lax.broadcasted_iota(jnp.int32, square, 1)
    )
    rows = op_rows(dot_rows(eye, op_ref[...].astype(F32).astype(BF16)), 0, SLOTS)
    chosen = operator_masks(rows, SLOTS)
    place = lax.broadcasted_iota(jnp.int32, (LEAVES, BLOCKS), 1)
    parity = parity_ref[0]
    for number in range(3):
        wanted = place + (number + parity * (2 - 2 * number)) * BLOCKS
        hits = jnp.concatenate(
            [one_hot(codes[:, s : s + 1], wanted) for s in range(SLOTS)], axis=0
        )
        counts_ref[number] = dot(chosen, hits).astype(BF16)


def eval_tables(rows_ref, cols_ref, left_ref, right_high_ref, right_low_ref):
    harmonics, side = rows_ref.shape
    rows = jnp.concatenate([rows_ref[...]] * 4, axis=0)
    rows = jnp.where(
        lax.broadcasted_iota(jnp.int32, rows.shape, 0) // harmonics
        == lax.broadcasted_iota(jnp.int32, rows.shape, 1) // (side // 4),
        rows,
        0.0,
    )
    high, low = halves(rows.T)
    left_ref[...] = jnp.concatenate([high, high, low, low], axis=1)
    for ref, part in zip((right_high_ref, right_low_ref), halves(cols_ref[...])):
        ref[...] = jnp.zeros_like(ref)
        for row in range(harmonics):
            ref[row * harmonics : (row + 1) * harmonics, row * side : (row + 1) * side] = part


def column_of(ref):
    side = ref.shape[0]
    leaf = lax.broadcasted_iota(jnp.int32, (LEAVES, side), 0)
    place = lax.broadcasted_iota(jnp.int32, (LEAVES, side), 1)
    spread = dot(one_hot(leaf // side, place), ref[...].astype(F32).astype(BF16))
    kept = jnp.where(leaf % side == place, spread, 0.0)
    return jnp.sum(kept, axis=1, keepdims=True).astype(jnp.int32)


def ready_kernel(
    parity_ref,
    src_ref,
    kind_ref,
    count_ref,
    density_ref,
    kinds_ref,
    list_ref,
    op_ref,
    rows_ref,
    cols_ref,
    out_ref,
    counts_ref,
    left_ref,
    right_high_ref,
    right_low_ref,
    products,
):
    near_field(src_ref, kind_ref, count_ref, density_ref, kinds_ref, out_ref, products)
    count_tables(parity_ref, list_ref, op_ref, counts_ref)
    eval_tables(rows_ref, cols_ref, left_ref, right_high_ref, right_low_ref)


def parent_kernel(own_ref, gathered_ref, shift_ref, window_ref, parents_ref):
    peers = gathered_ref.shape[0]
    flat = (peers * LEAVES, HALF)
    sources = jnp.concatenate(
        [
            gathered_ref[:, :LEAVES, :].reshape(flat),
            gathered_ref[:, LEAVES : 2 * LEAVES, :].reshape(flat),
        ],
        axis=1,
    )
    labels = []
    for peer in range(peers):
        numbers = gathered_ref[peer, 2 * LEAVES :, :].astype(F32)
        labels.append(numbers[0:1, :LEAVES] + numbers[1:2, :LEAVES] * float(PARENTS))
    labels = jnp.concatenate(labels, axis=1).astype(jnp.int32)
    positions = lax.broadcasted_iota(jnp.int32, (PARENTS, peers * LEAVES), 0)
    ordered = [
        dot(one_hot(labels, positions + octant * PARENTS), sources).astype(BF16)
        for octant in range(OCTANTS)
    ]
    total = jnp.zeros((PARENTS, COEFFS), F32)
    for octant in range(OCTANTS):
        total = total + dot(ordered[octant], shift_ref[octant])
    parents = total.astype(BF16)
    parents_ref[...] = parents
    window_ref[:PARENTS, :] = parents
    own = own_ref[0]
    for place in range(3):
        peer = lax.rem(own + place + peers - 1, peers)
        rows = slice(PARENTS + place * LEAVES, PARENTS + (place + 1) * LEAVES)
        window_ref[rows, :HALF] = gathered_ref[peer, :LEAVES, :]
        window_ref[rows, HALF:] = gathered_ref[peer, LEAVES : 2 * LEAVES, :]


def op_rows(numbers, first, slots):
    rows = [numbers[first + slot : first + slot + 1, :] for slot in range(slots)]
    return jnp.concatenate(rows, axis=1)


def operator_masks(rows, slots):
    shape = (LEAVES, slots * LEAVES)
    same = (lax.broadcasted_iota(jnp.int32, shape, 1) % LEAVES) == lax.broadcasted_iota(
        jnp.int32, shape, 0
    )
    diagonal = jnp.where(same, rows, -1.0)
    return jnp.concatenate([one_hot(diagonal, float(op)) for op in range(OPS)], axis=0)


def pick_table():
    shape = (16, COEFFS)
    row = lax.broadcasted_iota(jnp.int32, shape, 0)
    lane = lax.broadcasted_iota(jnp.int32, shape, 1)
    part, slot = lane // LEAVES, lane % PSLOTS
    value = jnp.where(part == 0, 128.0, 1.0)
    hit = (part < 2) & (row == slot) | (part == 2) & (row == slot + PSLOTS)
    return jnp.where(hit, value, 0.0).astype(BF16)


def coarse_kernel(
    parity_ref,
    parent_ref,
    gathered_ref,
    own_ref,
    counts_ref,
    leaf_ref,
    hits_ref,
    masks_ref,
):
    leaf_ref[...] = dot(counts_ref[1], own_ref[PARENTS:, :])
    peers = gathered_ref.shape[0]
    parent_of = column_of(parent_ref)
    pick = pick_table()
    lists = []
    for peer in range(peers):
        numbers = gathered_ref[peer, 2 * LEAVES :, :].astype(F32)
        lists.append(jnp.concatenate([numbers[2:3], numbers[3:4]], axis=1))
    lists = jnp.concatenate(lists, axis=0).astype(BF16)
    owner = one_hot(parent_of // 8, lax.broadcasted_iota(jnp.int32, (LEAVES, peers), 1))
    entries = dot(owner, lists)
    lane = lax.broadcasted_iota(jnp.int32, (LEAVES, COEFFS), 1)
    entries = jnp.where((lane % LEAVES) // 8 == parent_of % 8, entries, 0.0).astype(BF16)
    by_leaf = dot_rows(entries, pick).astype(jnp.int32)
    by_slot = dot_rows(pick, entries)
    masks_ref[...] = operator_masks(op_rows(by_slot, PSLOTS, PSLOTS), PSLOTS)
    column = lax.broadcasted_iota(jnp.int32, (LEAVES, PARENTS), 1)
    parity = parity_ref[0]
    for number in range(5):
        wanted = column + (number + parity * (4 - 2 * number)) * PARENTS
        hits_ref[:, number * PARENTS : (number + 1) * PARENTS] = jnp.concatenate(
            [one_hot(by_leaf[:, s : s + 1], wanted) for s in range(PSLOTS)], axis=0
        )


def final_kernel(
    octant_ref,
    counts_ref,
    leaf_ref,
    hits_ref,
    masks_ref,
    own_ref,
    near2_ref,
    near1_ref,
    mate_ref,
    far2_ref,
    operators_ref,
    shift_ref,
    left_ref,
    right_high_ref,
    right_low_ref,
    near_ref,
    out_ref,
    staged,
):
    leaf_sums = (
        leaf_ref[...]
        + dot(counts_ref[0], near1_ref[PARENTS:, :])
        + dot(counts_ref[2], mate_ref[PARENTS:, :])
    )
    sources = jnp.concatenate(
        [
            near2_ref[...],
            near1_ref[:PARENTS, :],
            own_ref[:PARENTS, :],
            mate_ref[:PARENTS, :],
            far2_ref[...],
        ],
        axis=0,
    )
    coarse_sums = dot(masks_ref[...], dot(hits_ref[...], sources).astype(BF16))
    leaf_high, leaf_low = halves(leaf_sums)
    coarse_high, coarse_low = halves(coarse_sums)
    total = jnp.zeros((4 * LEAVES, COEFFS), F32)
    for op in range(OPS):
        rows = slice(op * LEAVES, (op + 1) * LEAVES)
        stacked = jnp.concatenate(
            [leaf_high[rows], leaf_low[rows], coarse_high[rows], coarse_low[rows]], axis=0
        )
        total = total + dot(stacked, operators_ref[op])
    local = total[:LEAVES] + total[LEAVES : 2 * LEAVES]
    coarse_local = total[2 * LEAVES : 3 * LEAVES] + total[3 * LEAVES :]
    coarse_local = coarse_local.astype(BF16).astype(F32)
    octant_of = column_of(octant_ref)
    for octant in range(OCTANTS):
        chosen = jnp.where(octant_of == octant, coarse_local, 0.0).astype(BF16)
        local = local + dot_rows(chosen, shift_ref[octant])

    high, low = halves(local)
    spread = dot(jnp.concatenate([high, low], axis=0), right_high_ref[...])
    spread = spread[:LEAVES] + spread[LEAVES:] + dot(high, right_low_ref[...])
    harmonics = 16
    side = out_ref.shape[1]
    for row in range(harmonics):
        staged[pl.ds(row, LEAVES, stride=harmonics), :] = spread[:, row * side : (row + 1) * side]
    left = left_ref[...]
    for pair in range(out_ref.shape[0] // 2):
        parts = []
        for tile in (2 * pair, 2 * pair + 1):
            tile_high, tile_low = halves(staged[tile * LEAVES : (tile + 1) * LEAVES, :])
            parts.append(jnp.concatenate([tile_high, tile_low, tile_high, tile_low], axis=0))
        far = dot(left, jnp.concatenate(parts, axis=1))
        for half, tile in enumerate((2 * pair, 2 * pair + 1)):
            out_ref[tile] = (near_ref[tile] + far[:, half * side : (half + 1) * side]).astype(BF16)


VMEM = pl.BlockSpec(memory_space=pltpu.VMEM)
SMEM = pl.BlockSpec(memory_space=pltpu.SMEM)
HBM = pl.BlockSpec(memory_space=pltpu.HBM)


def ready_call(*operands):
    density, kinds = operands[4:6]
    tiles, side, _ = density.shape
    right = jax.ShapeDtypeStruct((COEFFS, 16 * side), BF16)
    return pl.pallas_call(
        ready_kernel,
        name="ready",
        out_shape=(
            jax.ShapeDtypeStruct((tiles, side, side), F32),
            jax.ShapeDtypeStruct((3, OPS * LEAVES, BLOCKS), BF16),
            jax.ShapeDtypeStruct((side, 4 * LEAVES), BF16),
            right,
            right,
        ),
        in_specs=[SMEM] * 4 + [VMEM] * 6,
        out_specs=(VMEM,) * 5,
        scratch_shapes=[pltpu.VMEM((tiles, kinds.shape[0], side, side), F32)],
        compiler_params=pltpu.CompilerParams(vmem_limit_bytes=67043328 - 4 * MIB // 2),
        cost_estimate=pl.CostEstimate(
            flops=8 * 10**9, bytes_accessed=6 * MIB, transcendentals=0
        ),
    )(*operands)


def payload_call(peers, *operands):
    return pl.pallas_call(
        payload_kernel,
        name="payload",
        out_shape=jax.ShapeDtypeStruct((peers, ROWS, HALF), BF16),
        in_specs=[HBM] * len(operands),
        out_specs=HBM,
        scratch_shapes=[pltpu.VMEM(operand.shape, operand.dtype) for operand in operands]
        + [
            pltpu.VMEM((ROWS, HALF), BF16),
            pltpu.SemaphoreType.DMA((len(operands),)),
            pltpu.SemaphoreType.DMA((2, peers)),
        ],
        compiler_params=pltpu.CompilerParams(vmem_limit_bytes=67043328),
        cost_estimate=pl.CostEstimate(
            flops=10**9, bytes_accessed=MIB, transcendentals=0
        ),
    )(*operands)


def parent_call(own, gathered, shift_up):
    return pl.pallas_call(
        parent_kernel,
        name="parents",
        out_shape=(
            jax.ShapeDtypeStruct((PARENTS + BLOCKS, COEFFS), BF16),
            jax.ShapeDtypeStruct((PARENTS, COEFFS), BF16),
        ),
        in_specs=[SMEM, VMEM, VMEM],
        out_specs=(VMEM, VMEM),
        compiler_params=pltpu.CompilerParams(vmem_limit_bytes=12 * MIB),
        cost_estimate=pl.CostEstimate(
            flops=2 * 10**9, bytes_accessed=2 * MIB, transcendentals=0
        ),
    )(own, gathered, shift_up)


def coarse_call(*operands):
    rows = OPS * LEAVES
    return pl.pallas_call(
        coarse_kernel,
        name="coarse",
        out_shape=(
            jax.ShapeDtypeStruct((rows, COEFFS), F32),
            jax.ShapeDtypeStruct((PSLOTS * LEAVES, 5 * PARENTS), BF16),
            jax.ShapeDtypeStruct((rows, PSLOTS * LEAVES), BF16),
        ),
        in_specs=[SMEM] + [VMEM] * (len(operands) - 1),
        out_specs=(VMEM, VMEM, VMEM),
        compiler_params=pltpu.CompilerParams(vmem_limit_bytes=16 * MIB),
        cost_estimate=pl.CostEstimate(
            flops=1000000000, bytes_accessed=4 * MIB, transcendentals=0
        ),
    )(*operands)


def final_call(*operands):
    near = operands[-1]
    return pl.pallas_call(
        final_kernel,
        name="final",
        out_shape=jax.ShapeDtypeStruct(near.shape, BF16),
        in_specs=[VMEM] * len(operands),
        out_specs=VMEM,
        scratch_shapes=[pltpu.VMEM((LEAVES * 16, near.shape[1]), F32)],
        compiler_params=pltpu.CompilerParams(vmem_limit_bytes=20 * MIB),
        cost_estimate=pl.CostEstimate(
            flops=4 * 10**9, bytes_accessed=8 * MIB, transcendentals=0
        ),
    )(*operands)


def routed(value, axis, to_even, to_odd):
    peers = lax.axis_size(axis)
    route = [(i, (i + (to_odd if i % 2 else to_even)) % peers) for i in range(peers)]
    return lax.ppermute(value, axis, route)


def body(
    leaf_moments,
    leaf_list,
    leaf_op,
    leaf_parent,
    leaf_octant,
    parent_list,
    parent_op,
    operators,
    shift_up,
    density,
    nearby_coulomb_kernel,
    near_src,
    near_kind,
    near_count,
    eval_rows,
    eval_cols,
):
    own = lax.axis_index("yz").astype(jnp.int32).reshape(1)
    parity = (lax.axis_index("gx") % 2).astype(jnp.int32).reshape(1)
    sent = payload_call(
        lax.axis_size("yz"),
        leaf_moments.reshape(LEAVES, COEFFS),
        leaf_parent,
        leaf_octant,
        parent_list[0],
        parent_op[0],
    )
    gathered = lax.all_to_all(sent, "yz", split_axis=0, concat_axis=0, tiled=True)

    near, counts, left, right_high, right_low = ready_call(
        parity,
        near_src,
        near_kind,
        near_count,
        density,
        nearby_coulomb_kernel,
        leaf_list.reshape(LEAVES, SLOTS),
        leaf_op.reshape(LEAVES, SLOTS),
        eval_rows.T,
        eval_cols,
    )

    window, parents = parent_call(own, gathered, shift_up)
    near1 = routed(window, "gx", -1, 1)
    near2 = routed(parents, "gx", 2, -2)
    far2 = routed(parents, "gx", -2, 2)
    mate = routed(window, "gx", 1, -1)
    leaf, hits, masks = coarse_call(
        parity, leaf_parent, gathered, window, counts
    )
    return final_call(
        leaf_octant,
        counts,
        leaf,
        hits,
        masks,
        window,
        near2,
        near1,
        mate,
        far2,
        operators,
        shift_up,
        left,
        right_high,
        right_low,
        near,
    )


def solution(mesh):
    in_specs = (
        P("gx", "yz", None),
        P("gx", "yz", None),
        P("gx", "yz", None),
        P("gx", "yz"),
        P("gx", "yz"),
        P("gx", "yz", None),
        P("gx", "yz", None),
        P(),
        P(),
        P(("gx", "yz"), None, None),
        P(),
        P(("gx", "yz"), None),
        P(("gx", "yz"), None),
        P(("gx", "yz")),
        P(),
        P(),
    )
    out_specs = P(("gx", "yz"), None, None)
    return jax.shard_map(body, mesh=mesh, in_specs=in_specs, out_specs=out_specs, check_vma=False)
```

```python
import jax
import jax.numpy as jnp
from jax import lax
from jax.experimental import pallas as pl
from jax.experimental.pallas import tpu as pltpu
from jax.sharding import PartitionSpec as P

BF16 = jnp.bfloat16
F32 = jnp.float32
LEAVES = 64
ROWS = 136
COEFFS = 256
HALF = 128
BLOCKS = 3 * LEAVES
PARENTS = 128
OPS = 16
OCTANTS = 8
SLOTS = 16
PSLOTS = 8
MIB = 1024 * 1024


def dot(a, b):
    return jnp.dot(a, b, preferred_element_type=F32)


def dot_rows(a, b):
    return lax.dot_general(a, b, (((1,), (1,)), ((), ())), preferred_element_type=F32)


def one_hot(labels, positions):
    return jnp.where(labels == positions, 1.0, 0.0).astype(BF16)


def halves(x):
    high = x.astype(BF16)
    return high, (x - high.astype(F32)).astype(BF16)


def near_field(src_ref, kind_ref, count_ref, density_ref, kinds_ref, out_ref, products):
    kinds_count, side, _ = kinds_ref.shape
    tiles = density_ref.shape[0]
    stacked = kinds_ref[...].reshape(kinds_count * side, side)

    @pl.loop(0, tiles // 2)
    def _(pair):
        both = jnp.concatenate([density_ref[2 * pair], density_ref[2 * pair + 1]], axis=1)
        made = dot(stacked, both)
        for half in range(2):
            products[2 * pair + half] = made[:, half * side : (half + 1) * side].reshape(
                kinds_count, side, side
            )

    @pl.loop(0, tiles)
    def _(tile):
        def add(slot, total):
            return total + products[src_ref[tile, slot], kind_ref[tile, slot]]

        out_ref[tile] = lax.fori_loop(
            0, count_ref[tile], add, jnp.zeros((side, side), F32)
        )


def payload_kernel(*refs):
    sources, out_ref, held, block, in_sem, out_sem = refs[:5], refs[5], refs[6:11], *refs[11:]
    fetches = [
        pltpu.make_async_copy(source, target, in_sem.at[number])
        for number, (source, target) in enumerate(zip(sources, held))
    ]
    for fetch in fetches:
        fetch.start()
    fetches[0].wait()
    moments_ref, parent_ref, octant_ref, list_ref, op_ref = held
    block[:LEAVES, :] = moments_ref[:, :HALF]
    block[LEAVES : 2 * LEAVES, :] = moments_ref[:, HALF:]
    peers = out_ref.shape[0]
    stores = []
    for part, rows in enumerate((slice(0, 2 * LEAVES), slice(2 * LEAVES, ROWS))):
        stores.append(
            [
                pltpu.make_async_copy(
                    block.at[rows], out_ref.at[peer, rows], out_sem.at[part, peer]
                )
                for peer in range(peers)
            ]
        )
    for store in stores[0]:
        store.start()
    for fetch in fetches[1:]:
        fetch.wait()
    coarse = list_ref[...]
    numbers = jnp.concatenate(
        [parent_ref[...], octant_ref[...], coarse >> 7, coarse & 127, op_ref[...]], axis=0
    )
    count, side = numbers.shape
    lane = lax.broadcasted_iota(jnp.int32, (side, LEAVES), 1)
    spread = dot(
        numbers.astype(F32).astype(BF16),
        one_hot(lane % side, lax.broadcasted_iota(jnp.int32, (side, LEAVES), 0)),
    )
    lane = lax.broadcasted_iota(jnp.int32, (count, LEAVES), 1)
    row = lax.broadcasted_iota(jnp.int32, (count, LEAVES), 0)
    kept = jnp.where(lane // side == row % side, spread, 0.0)
    rows = [
        jnp.sum(kept[number * side : (number + 1) * side], axis=0, keepdims=True)
        for number in range(count // side)
    ]
    blank = jnp.zeros((1, LEAVES), F32)
    lines = [
        jnp.concatenate(pair, axis=1)
        for pair in ((rows[0], blank), (rows[1], blank), (rows[2], rows[3]), (rows[4], blank))
    ]
    lines = jnp.concatenate(lines + [jnp.zeros((4, 2 * LEAVES), F32)], axis=0).astype(BF16)
    block[2 * LEAVES :, :] = lines
    for store in stores[1]:
        store.start()
    for store in stores[0] + stores[1]:
        store.wait()


def count_tables(parity_ref, list_ref, op_ref, counts_ref):
    leaf_list = list_ref[...]
    side = 8
    span = 2 * side + 1
    leaf = lax.broadcasted_iota(jnp.int32, leaf_list.shape, 0)
    first = leaf // side + leaf_list // span
    second = leaf % side + leaf_list % span
    codes = (
        (first // side) * BLOCKS
        + (second // side) * LEAVES
        + (first % side) * side
        + second % side
    )
    square = (SLOTS, SLOTS)
    eye = one_hot(
        lax.broadcasted_iota(jnp.int32, square, 0), lax.broadcasted_iota(jnp.int32, square, 1)
    )
    rows = op_rows(dot_rows(eye, op_ref[...].astype(F32).astype(BF16)), 0, SLOTS)
    chosen = operator_masks(rows, SLOTS)
    place = lax.broadcasted_iota(jnp.int32, (LEAVES, BLOCKS), 1)
    parity = parity_ref[0]
    for number in range(3):
        wanted = place + (number + parity * (2 - 2 * number)) * BLOCKS
        hits = jnp.concatenate(
            [one_hot(codes[:, s : s + 1], wanted) for s in range(SLOTS)], axis=0
        )
        counts_ref[number] = dot(chosen, hits).astype(BF16)


def eval_tables(rows_ref, cols_ref, left_ref, right_ref):
    harmonics, side = rows_ref.shape
    rows = jnp.concatenate([rows_ref[...]] * 4, axis=0)
    rows = jnp.where(
        lax.broadcasted_iota(jnp.int32, rows.shape, 0) // harmonics
        == lax.broadcasted_iota(jnp.int32, rows.shape, 1) // (side // 4),
        rows,
        0.0,
    )
    high, low = halves(rows.T)
    left_ref[...] = jnp.concatenate([high, high, low, low], axis=1)
    high, low = halves(cols_ref[...])
    right_ref[...] = jnp.zeros_like(right_ref)
    right_ref[:harmonics, :side] = high
    right_ref[:harmonics, side:] = low
    right_ref[side : side + harmonics, :side] = high


def column_of(ref):
    side = ref.shape[0]
    leaf = lax.broadcasted_iota(jnp.int32, (LEAVES, side), 0)
    place = lax.broadcasted_iota(jnp.int32, (LEAVES, side), 1)
    spread = dot(one_hot(leaf // side, place), ref[...].astype(F32).astype(BF16))
    kept = jnp.where(leaf % side == place, spread, 0.0)
    return jnp.sum(kept, axis=1, keepdims=True).astype(jnp.int32)


def ready_kernel(
    parity_ref,
    src_ref,
    kind_ref,
    count_ref,
    density_ref,
    kinds_ref,
    list_ref,
    op_ref,
    rows_ref,
    cols_ref,
    out_ref,
    counts_ref,
    left_ref,
    right_ref,
    products,
):
    near_field(src_ref, kind_ref, count_ref, density_ref, kinds_ref, out_ref, products)
    count_tables(parity_ref, list_ref, op_ref, counts_ref)
    eval_tables(rows_ref, cols_ref, left_ref, right_ref)


def parent_kernel(own_ref, gathered_ref, shift_ref, window_ref, parents_ref):
    peers = gathered_ref.shape[0]
    flat = (peers * LEAVES, HALF)
    sources = jnp.concatenate(
        [
            gathered_ref[:, :LEAVES, :].reshape(flat),
            gathered_ref[:, LEAVES : 2 * LEAVES, :].reshape(flat),
        ],
        axis=1,
    )
    labels = []
    for peer in range(peers):
        numbers = gathered_ref[peer, 2 * LEAVES :, :].astype(F32)
        labels.append(numbers[0:1, :LEAVES] + numbers[1:2, :LEAVES] * float(PARENTS))
    labels = jnp.concatenate(labels, axis=1).astype(jnp.int32)
    positions = lax.broadcasted_iota(jnp.int32, (PARENTS, peers * LEAVES), 0)
    ordered = [
        dot(one_hot(labels, positions + octant * PARENTS), sources).astype(BF16)
        for octant in range(OCTANTS)
    ]
    total = jnp.zeros((PARENTS, COEFFS), F32)
    for octant in range(OCTANTS):
        total = total + dot(ordered[octant], shift_ref[octant])
    parents = total.astype(BF16)
    parents_ref[...] = parents
    window_ref[:PARENTS, :] = parents
    own = own_ref[0]
    for place in range(3):
        peer = lax.rem(own + place + peers - 1, peers)
        rows = slice(PARENTS + place * LEAVES, PARENTS + (place + 1) * LEAVES)
        window_ref[rows, :HALF] = gathered_ref[peer, :LEAVES, :]
        window_ref[rows, HALF:] = gathered_ref[peer, LEAVES : 2 * LEAVES, :]


def op_rows(numbers, first, slots):
    rows = [numbers[first + slot : first + slot + 1, :] for slot in range(slots)]
    return jnp.concatenate(rows, axis=1)


def operator_masks(rows, slots):
    shape = (LEAVES, slots * LEAVES)
    same = (lax.broadcasted_iota(jnp.int32, shape, 1) % LEAVES) == lax.broadcasted_iota(
        jnp.int32, shape, 0
    )
    diagonal = jnp.where(same, rows, -1.0)
    return jnp.concatenate([one_hot(diagonal, float(op)) for op in range(OPS)], axis=0)


def pick_table():
    shape = (16, COEFFS)
    row = lax.broadcasted_iota(jnp.int32, shape, 0)
    lane = lax.broadcasted_iota(jnp.int32, shape, 1)
    part, slot = lane // LEAVES, lane % PSLOTS
    value = jnp.where(part == 0, 128.0, 1.0)
    hit = (part < 2) & (row == slot) | (part == 2) & (row == slot + PSLOTS)
    return jnp.where(hit, value, 0.0).astype(BF16)


def coarse_kernel(
    parity_ref,
    parent_ref,
    gathered_ref,
    own_ref,
    counts_ref,
    leaf_ref,
    hits_ref,
    masks_ref,
):
    leaf_ref[...] = dot(counts_ref[1], own_ref[PARENTS:, :])
    peers = gathered_ref.shape[0]
    parent_of = column_of(parent_ref)
    pick = pick_table()
    lists = []
    for peer in range(peers):
        numbers = gathered_ref[peer, 2 * LEAVES :, :].astype(F32)
        lists.append(jnp.concatenate([numbers[2:3], numbers[3:4]], axis=1))
    lists = jnp.concatenate(lists, axis=0).astype(BF16)
    owner = one_hot(parent_of // 8, lax.broadcasted_iota(jnp.int32, (LEAVES, peers), 1))
    entries = dot(owner, lists)
    lane = lax.broadcasted_iota(jnp.int32, (LEAVES, COEFFS), 1)
    entries = jnp.where((lane % LEAVES) // 8 == parent_of % 8, entries, 0.0).astype(BF16)
    by_leaf = dot_rows(entries, pick).astype(jnp.int32)
    by_slot = dot_rows(pick, entries)
    masks_ref[...] = operator_masks(op_rows(by_slot, PSLOTS, PSLOTS), PSLOTS)
    column = lax.broadcasted_iota(jnp.int32, (LEAVES, PARENTS), 1)
    parity = parity_ref[0]
    for number in range(5):
        wanted = column + (number + parity * (4 - 2 * number)) * PARENTS
        hits_ref[:, number * PARENTS : (number + 1) * PARENTS] = jnp.concatenate(
            [one_hot(by_leaf[:, s : s + 1], wanted) for s in range(PSLOTS)], axis=0
        )


def final_kernel(
    octant_ref,
    counts_ref,
    leaf_ref,
    hits_ref,
    masks_ref,
    own_ref,
    near2_ref,
    near1_ref,
    mate_ref,
    far2_ref,
    operators_ref,
    shift_ref,
    left_ref,
    right_ref,
    near_ref,
    out_ref,
    staged,
):
    leaf_sums = (
        leaf_ref[...]
        + dot(counts_ref[0], near1_ref[PARENTS:, :])
        + dot(counts_ref[2], mate_ref[PARENTS:, :])
    )
    sources = jnp.concatenate(
        [
            near2_ref[...],
            near1_ref[:PARENTS, :],
            own_ref[:PARENTS, :],
            mate_ref[:PARENTS, :],
            far2_ref[...],
        ],
        axis=0,
    )
    coarse_sums = dot(masks_ref[...], dot(hits_ref[...], sources).astype(BF16))
    leaf_high, leaf_low = halves(leaf_sums)
    coarse_high, coarse_low = halves(coarse_sums)
    total = jnp.zeros((4 * LEAVES, COEFFS), F32)
    for op in range(OPS):
        rows = slice(op * LEAVES, (op + 1) * LEAVES)
        stacked = jnp.concatenate(
            [leaf_high[rows], leaf_low[rows], coarse_high[rows], coarse_low[rows]], axis=0
        )
        total = total + dot(stacked, operators_ref[op])
    local = total[:LEAVES] + total[LEAVES : 2 * LEAVES]
    coarse_local = total[2 * LEAVES : 3 * LEAVES] + total[3 * LEAVES :]
    coarse_local = coarse_local.astype(BF16).astype(F32)
    octant_of = column_of(octant_ref)
    for octant in range(OCTANTS):
        chosen = jnp.where(octant_of == octant, coarse_local, 0.0).astype(BF16)
        local = local + dot_rows(chosen, shift_ref[octant])

    harmonics = 16
    side = out_ref.shape[1]
    for row in range(harmonics):
        first = row * harmonics
        block = local[:, first // side * side : first // side * side + side]
        if first % side:
            block = pltpu.roll(block, side - first % side, 1)
        staged[pl.ds(row, LEAVES, stride=harmonics), :] = block
    spread = dot(jnp.concatenate(halves(staged[...]), axis=1), right_ref[...])
    spread = spread[:, :side] + spread[:, side:]
    left = left_ref[...]
    for pair in range(out_ref.shape[0] // 2):
        parts = []
        for tile in (2 * pair, 2 * pair + 1):
            tile_high, tile_low = halves(spread[tile * LEAVES : (tile + 1) * LEAVES])
            parts.append(jnp.concatenate([tile_high, tile_low, tile_high, tile_low], axis=0))
        far = dot(left, jnp.concatenate(parts, axis=1))
        for half, tile in enumerate((2 * pair, 2 * pair + 1)):
            out_ref[tile] = (near_ref[tile] + far[:, half * side : (half + 1) * side]).astype(BF16)


VMEM = pl.BlockSpec(memory_space=pltpu.VMEM)
SMEM = pl.BlockSpec(memory_space=pltpu.SMEM)
HBM = pl.BlockSpec(memory_space=pltpu.HBM)


def ready_call(*operands):
    density, kinds = operands[4:6]
    tiles, side, _ = density.shape
    return pl.pallas_call(
        ready_kernel,
        name="ready",
        out_shape=(
            jax.ShapeDtypeStruct((tiles, side, side), F32),
            jax.ShapeDtypeStruct((3, OPS * LEAVES, BLOCKS), BF16),
            jax.ShapeDtypeStruct((side, 4 * LEAVES), BF16),
            jax.ShapeDtypeStruct((2 * side, 2 * side), BF16),
        ),
        in_specs=[SMEM] * 4 + [VMEM] * 6,
        out_specs=(VMEM,) * 4,
        scratch_shapes=[pltpu.VMEM((tiles, kinds.shape[0], side, side), F32)],
        compiler_params=pltpu.CompilerParams(vmem_limit_bytes=67043328 - 4 * MIB // 2),
        cost_estimate=pl.CostEstimate(
            flops=8 * 10**9, bytes_accessed=6 * MIB, transcendentals=0
        ),
    )(*operands)


def payload_call(peers, *operands):
    return pl.pallas_call(
        payload_kernel,
        name="payload",
        out_shape=jax.ShapeDtypeStruct((peers, ROWS, HALF), BF16),
        in_specs=[HBM] * len(operands),
        out_specs=HBM,
        scratch_shapes=[pltpu.VMEM(operand.shape, operand.dtype) for operand in operands]
        + [
            pltpu.VMEM((ROWS, HALF), BF16),
            pltpu.SemaphoreType.DMA((len(operands),)),
            pltpu.SemaphoreType.DMA((2, peers)),
        ],
        compiler_params=pltpu.CompilerParams(vmem_limit_bytes=67043328),
        cost_estimate=pl.CostEstimate(
            flops=10**9, bytes_accessed=MIB, transcendentals=0
        ),
    )(*operands)


def parent_call(own, gathered, shift_up):
    return pl.pallas_call(
        parent_kernel,
        name="parents",
        out_shape=(
            jax.ShapeDtypeStruct((PARENTS + BLOCKS, COEFFS), BF16),
            jax.ShapeDtypeStruct((PARENTS, COEFFS), BF16),
        ),
        in_specs=[SMEM, VMEM, VMEM],
        out_specs=(VMEM, VMEM),
        compiler_params=pltpu.CompilerParams(vmem_limit_bytes=12 * MIB),
        cost_estimate=pl.CostEstimate(
            flops=2 * 10**9, bytes_accessed=2 * MIB, transcendentals=0
        ),
    )(own, gathered, shift_up)


def coarse_call(*operands):
    rows = OPS * LEAVES
    return pl.pallas_call(
        coarse_kernel,
        name="coarse",
        out_shape=(
            jax.ShapeDtypeStruct((rows, COEFFS), F32),
            jax.ShapeDtypeStruct((PSLOTS * LEAVES, 5 * PARENTS), BF16),
            jax.ShapeDtypeStruct((rows, PSLOTS * LEAVES), BF16),
        ),
        in_specs=[SMEM] + [VMEM] * (len(operands) - 1),
        out_specs=(VMEM, VMEM, VMEM),
        compiler_params=pltpu.CompilerParams(vmem_limit_bytes=16 * MIB),
        cost_estimate=pl.CostEstimate(
            flops=1000000000, bytes_accessed=4 * MIB, transcendentals=0
        ),
    )(*operands)


def final_call(*operands):
    near = operands[-1]
    return pl.pallas_call(
        final_kernel,
        name="final",
        out_shape=jax.ShapeDtypeStruct(near.shape, BF16),
        in_specs=[VMEM] * len(operands),
        out_specs=VMEM,
        scratch_shapes=[pltpu.VMEM((LEAVES * 16, near.shape[1]), F32)],
        compiler_params=pltpu.CompilerParams(vmem_limit_bytes=20 * MIB),
        cost_estimate=pl.CostEstimate(
            flops=4 * 10**9, bytes_accessed=8 * MIB, transcendentals=0
        ),
    )(*operands)


def routed(value, axis, to_even, to_odd):
    peers = lax.axis_size(axis)
    route = [(i, (i + (to_odd if i % 2 else to_even)) % peers) for i in range(peers)]
    return lax.ppermute(value, axis, route)


def body(
    leaf_moments,
    leaf_list,
    leaf_op,
    leaf_parent,
    leaf_octant,
    parent_list,
    parent_op,
    operators,
    shift_up,
    density,
    nearby_coulomb_kernel,
    near_src,
    near_kind,
    near_count,
    eval_rows,
    eval_cols,
):
    own = lax.axis_index("yz").astype(jnp.int32).reshape(1)
    parity = (lax.axis_index("gx") % 2).astype(jnp.int32).reshape(1)
    sent = payload_call(
        lax.axis_size("yz"),
        leaf_moments.reshape(LEAVES, COEFFS),
        leaf_parent,
        leaf_octant,
        parent_list[0],
        parent_op[0],
    )
    gathered = lax.all_to_all(sent, "yz", split_axis=0, concat_axis=0, tiled=True)

    near, counts, left, right = ready_call(
        parity,
        near_src,
        near_kind,
        near_count,
        density,
        nearby_coulomb_kernel,
        leaf_list.reshape(LEAVES, SLOTS),
        leaf_op.reshape(LEAVES, SLOTS),
        eval_rows.T,
        eval_cols,
    )

    window, parents = parent_call(own, gathered, shift_up)
    near1 = routed(window, "gx", -1, 1)
    far2 = routed(parents, "gx", -2, 2)
    near2 = routed(parents, "gx", 2, -2)
    mate = routed(window, "gx", 1, -1)
    leaf, hits, masks = coarse_call(
        parity, leaf_parent, gathered, window, counts
    )
    return final_call(
        leaf_octant,
        counts,
        leaf,
        hits,
        masks,
        window,
        near2,
        near1,
        mate,
        far2,
        operators,
        shift_up,
        left,
        right,
        near,
    )


def solution(mesh):
    in_specs = (
        P("gx", "yz", None),
        P("gx", "yz", None),
        P("gx", "yz", None),
        P("gx", "yz"),
        P("gx", "yz"),
        P("gx", "yz", None),
        P("gx", "yz", None),
        P(),
        P(),
        P(("gx", "yz"), None, None),
        P(),
        P(("gx", "yz"), None),
        P(("gx", "yz"), None),
        P(("gx", "yz")),
        P(),
        P(),
    )
    out_specs = P(("gx", "yz"), None, None)
    return jax.shard_map(body, mesh=mesh, in_specs=in_specs, out_specs=out_specs, check_vma=False)
```

```python
import jax
import jax.numpy as jnp
from jax import lax
from jax.experimental import pallas as pl
from jax.experimental.pallas import tpu as pltpu
from jax.sharding import PartitionSpec as P

BF16 = jnp.bfloat16
F32 = jnp.float32
LEAVES = 64
ROWS = 136
COEFFS = 256
HALF = 128
BLOCKS = 3 * LEAVES
PARENTS = 128
OPS = 16
OCTANTS = 8
SLOTS = 16
PSLOTS = 8
MIB = 1024 * 1024


def dot(a, b):
    return jnp.dot(a, b, preferred_element_type=F32)


def dot_rows(a, b):
    return lax.dot_general(a, b, (((1,), (1,)), ((), ())), preferred_element_type=F32)


def one_hot(labels, positions):
    return jnp.where(labels == positions, 1.0, 0.0).astype(BF16)


def halves(x):
    high = x.astype(BF16)
    return high, (x - high.astype(F32)).astype(BF16)


def near_field(src_ref, kind_ref, count_ref, density_ref, kinds_ref, out_ref, products):
    kinds_count, side, _ = kinds_ref.shape
    tiles = density_ref.shape[0]
    stacked = kinds_ref[...].reshape(kinds_count * side, side)

    @pl.loop(0, tiles // 2)
    def _(pair):
        both = jnp.concatenate([density_ref[2 * pair], density_ref[2 * pair + 1]], axis=1)
        made = dot(stacked, both)
        for half in range(2):
            products[2 * pair + half] = made[:, half * side : (half + 1) * side].reshape(
                kinds_count, side, side
            )

    @pl.loop(0, tiles)
    def _(tile):
        def add(slot, total):
            return total + products[src_ref[tile, slot], kind_ref[tile, slot]]

        out_ref[tile] = lax.fori_loop(
            0, count_ref[tile], add, jnp.zeros((side, side), F32)
        )


def payload_kernel(*refs):
    sources, out_ref, held, block, in_sem, out_sem = refs[:5], refs[5], refs[6:11], *refs[11:]
    fetches = [
        pltpu.make_async_copy(source, target, in_sem.at[number])
        for number, (source, target) in enumerate(zip(sources, held))
    ]
    for fetch in fetches:
        fetch.start()
    fetches[0].wait()
    moments_ref, parent_ref, octant_ref, list_ref, op_ref = held
    block[:LEAVES, :] = moments_ref[:, :HALF]
    block[LEAVES : 2 * LEAVES, :] = moments_ref[:, HALF:]
    peers = out_ref.shape[0]
    stores = []
    for part, rows in enumerate((slice(0, 2 * LEAVES), slice(2 * LEAVES, ROWS))):
        stores.append(
            [
                pltpu.make_async_copy(
                    block.at[rows], out_ref.at[peer, rows], out_sem.at[part, peer]
                )
                for peer in range(peers)
            ]
        )
    for store in stores[0]:
        store.start()
    for fetch in fetches[1:]:
        fetch.wait()
    coarse = list_ref[...]
    numbers = jnp.concatenate(
        [parent_ref[...], octant_ref[...], coarse >> 7, coarse & 127, op_ref[...]], axis=0
    )
    count, side = numbers.shape
    lane = lax.broadcasted_iota(jnp.int32, (side, LEAVES), 1)
    spread = dot(
        numbers.astype(F32).astype(BF16),
        one_hot(lane % side, lax.broadcasted_iota(jnp.int32, (side, LEAVES), 0)),
    )
    lane = lax.broadcasted_iota(jnp.int32, (count, LEAVES), 1)
    row = lax.broadcasted_iota(jnp.int32, (count, LEAVES), 0)
    kept = jnp.where(lane // side == row % side, spread, 0.0)
    rows = [
        jnp.sum(kept[number * side : (number + 1) * side], axis=0, keepdims=True)
        for number in range(count // side)
    ]
    blank = jnp.zeros((1, LEAVES), F32)
    lines = [
        jnp.concatenate(pair, axis=1)
        for pair in ((rows[0], blank), (rows[1], blank), (rows[2], rows[3]), (rows[4], blank))
    ]
    lines = jnp.concatenate(lines + [jnp.zeros((4, 2 * LEAVES), F32)], axis=0).astype(BF16)
    block[2 * LEAVES :, :] = lines
    for store in stores[1]:
        store.start()
    for store in stores[0] + stores[1]:
        store.wait()


def count_tables(parity_ref, list_ref, op_ref, counts_ref):
    leaf_list = list_ref[...]
    side = 8
    span = 2 * side + 1
    leaf = lax.broadcasted_iota(jnp.int32, leaf_list.shape, 0)
    first = leaf // side + leaf_list // span
    second = leaf % side + leaf_list % span
    codes = (
        (first // side) * BLOCKS
        + (second // side) * LEAVES
        + (first % side) * side
        + second % side
    )
    square = (SLOTS, SLOTS)
    eye = one_hot(
        lax.broadcasted_iota(jnp.int32, square, 0), lax.broadcasted_iota(jnp.int32, square, 1)
    )
    rows = op_rows(dot_rows(eye, op_ref[...].astype(F32).astype(BF16)), 0, SLOTS)
    chosen = operator_masks(rows, SLOTS)
    place = lax.broadcasted_iota(jnp.int32, (LEAVES, BLOCKS), 1)
    parity = parity_ref[0]
    for number in range(3):
        wanted = place + (number + parity * (2 - 2 * number)) * BLOCKS
        hits = jnp.concatenate(
            [one_hot(codes[:, s : s + 1], wanted) for s in range(SLOTS)], axis=0
        )
        counts_ref[number] = dot(chosen, hits).astype(BF16)


def eval_tables(rows_ref, cols_ref, left_ref, right_ref):
    harmonics, side = rows_ref.shape
    rows = jnp.concatenate([rows_ref[...]] * 4, axis=0)
    rows = jnp.where(
        lax.broadcasted_iota(jnp.int32, rows.shape, 0) // harmonics
        == lax.broadcasted_iota(jnp.int32, rows.shape, 1) // (side // 4),
        rows,
        0.0,
    )
    high, low = halves(rows.T)
    left_ref[...] = jnp.concatenate([high, high, low, low], axis=1)
    high, low = halves(cols_ref[...])
    right_ref[...] = jnp.zeros_like(right_ref)
    right_ref[:harmonics, :side] = high
    right_ref[:harmonics, side:] = low
    right_ref[side : side + harmonics, :side] = high


def column_of(ref):
    side = ref.shape[0]
    leaf = lax.broadcasted_iota(jnp.int32, (LEAVES, side), 0)
    place = lax.broadcasted_iota(jnp.int32, (LEAVES, side), 1)
    spread = dot(one_hot(leaf // side, place), ref[...].astype(F32).astype(BF16))
    kept = jnp.where(leaf % side == place, spread, 0.0)
    return jnp.sum(kept, axis=1, keepdims=True).astype(jnp.int32)


def ready_kernel(
    parity_ref,
    src_ref,
    kind_ref,
    count_ref,
    density_ref,
    kinds_ref,
    list_ref,
    op_ref,
    rows_ref,
    cols_ref,
    out_ref,
    counts_ref,
    left_ref,
    right_ref,
    products,
):
    near_field(src_ref, kind_ref, count_ref, density_ref, kinds_ref, out_ref, products)
    count_tables(parity_ref, list_ref, op_ref, counts_ref)
    eval_tables(rows_ref, cols_ref, left_ref, right_ref)


def parent_kernel(own_ref, gathered_ref, shift_ref, window_ref, parents_ref):
    peers = gathered_ref.shape[0]
    flat = (peers * LEAVES, HALF)
    sources = jnp.concatenate(
        [
            gathered_ref[:, :LEAVES, :].reshape(flat),
            gathered_ref[:, LEAVES : 2 * LEAVES, :].reshape(flat),
        ],
        axis=1,
    )
    labels = []
    for peer in range(peers):
        numbers = gathered_ref[peer, 2 * LEAVES :, :].astype(F32)
        labels.append(numbers[0:1, :LEAVES] + numbers[1:2, :LEAVES] * float(PARENTS))
    labels = jnp.concatenate(labels, axis=1).astype(jnp.int32)
    positions = lax.broadcasted_iota(jnp.int32, (PARENTS, peers * LEAVES), 0)
    ordered = [
        dot(one_hot(labels, positions + octant * PARENTS), sources).astype(BF16)
        for octant in range(OCTANTS)
    ]
    total = jnp.zeros((PARENTS, COEFFS), F32)
    for octant in range(OCTANTS):
        total = total + dot(ordered[octant], shift_ref[octant])
    parents = total.astype(BF16)
    parents_ref[...] = parents
    window_ref[:PARENTS, :] = parents
    own = own_ref[0]
    for place in range(3):
        peer = lax.rem(own + place + peers - 1, peers)
        rows = slice(PARENTS + place * LEAVES, PARENTS + (place + 1) * LEAVES)
        window_ref[rows, :HALF] = gathered_ref[peer, :LEAVES, :]
        window_ref[rows, HALF:] = gathered_ref[peer, LEAVES : 2 * LEAVES, :]


def op_rows(numbers, first, slots):
    rows = [numbers[first + slot : first + slot + 1, :] for slot in range(slots)]
    return jnp.concatenate(rows, axis=1)


def operator_masks(rows, slots):
    shape = (LEAVES, slots * LEAVES)
    same = (lax.broadcasted_iota(jnp.int32, shape, 1) % LEAVES) == lax.broadcasted_iota(
        jnp.int32, shape, 0
    )
    diagonal = jnp.where(same, rows, -1.0)
    return jnp.concatenate([one_hot(diagonal, float(op)) for op in range(OPS)], axis=0)


def pick_table():
    shape = (16, COEFFS)
    row = lax.broadcasted_iota(jnp.int32, shape, 0)
    lane = lax.broadcasted_iota(jnp.int32, shape, 1)
    part, slot = lane // LEAVES, lane % PSLOTS
    value = jnp.where(part == 0, 128.0, 1.0)
    hit = (part < 2) & (row == slot) | (part == 2) & (row == slot + PSLOTS)
    return jnp.where(hit, value, 0.0).astype(BF16)


def coarse_kernel(
    parity_ref,
    parent_ref,
    gathered_ref,
    own_ref,
    counts_ref,
    leaf_ref,
    hits_ref,
    masks_ref,
):
    leaf_ref[...] = dot(counts_ref[1], own_ref[PARENTS:, :])
    peers = gathered_ref.shape[0]
    parent_of = column_of(parent_ref)
    pick = pick_table()
    lists = []
    for peer in range(peers):
        numbers = gathered_ref[peer, 2 * LEAVES :, :].astype(F32)
        lists.append(jnp.concatenate([numbers[2:3], numbers[3:4]], axis=1))
    lists = jnp.concatenate(lists, axis=0).astype(BF16)
    owner = one_hot(parent_of // 8, lax.broadcasted_iota(jnp.int32, (LEAVES, peers), 1))
    entries = dot(owner, lists)
    lane = lax.broadcasted_iota(jnp.int32, (LEAVES, COEFFS), 1)
    entries = jnp.where((lane % LEAVES) // 8 == parent_of % 8, entries, 0.0).astype(BF16)
    by_leaf = dot_rows(entries, pick).astype(jnp.int32)
    by_slot = dot_rows(pick, entries)
    masks_ref[...] = operator_masks(op_rows(by_slot, PSLOTS, PSLOTS), PSLOTS)
    column = lax.broadcasted_iota(jnp.int32, (LEAVES, PARENTS), 1)
    parity = parity_ref[0]
    for number in range(5):
        wanted = column + (number + parity * (4 - 2 * number)) * PARENTS
        hits_ref[:, number * PARENTS : (number + 1) * PARENTS] = jnp.concatenate(
            [one_hot(by_leaf[:, s : s + 1], wanted) for s in range(PSLOTS)], axis=0
        )


def operated(sums, operators_ref):
    high, low = halves(sums)
    total = jnp.zeros((2 * LEAVES, COEFFS), F32)
    for op in range(OPS):
        rows = slice(op * LEAVES, (op + 1) * LEAVES)
        total = total + dot(
            jnp.concatenate([high[rows], low[rows]], axis=0), operators_ref[op]
        )
    return total[:LEAVES] + total[LEAVES:]


def leaf_kernel(counts_ref, leaf_ref, near1_ref, mate_ref, operators_ref, local_ref):
    leaf_sums = (
        leaf_ref[...]
        + dot(counts_ref[0], near1_ref[PARENTS:, :])
        + dot(counts_ref[2], mate_ref[PARENTS:, :])
    )
    local_ref[...] = operated(leaf_sums, operators_ref)


def final_kernel(
    octant_ref,
    local_ref,
    hits_ref,
    masks_ref,
    own_ref,
    near2_ref,
    near1_ref,
    mate_ref,
    far2_ref,
    operators_ref,
    shift_ref,
    left_ref,
    right_ref,
    near_ref,
    out_ref,
    staged,
):
    sources = jnp.concatenate(
        [
            near2_ref[...],
            near1_ref[:PARENTS, :],
            own_ref[:PARENTS, :],
            mate_ref[:PARENTS, :],
            far2_ref[...],
        ],
        axis=0,
    )
    coarse_sums = dot(masks_ref[...], dot(hits_ref[...], sources).astype(BF16))
    local = local_ref[...]
    coarse_local = operated(coarse_sums, operators_ref).astype(BF16).astype(F32)
    octant_of = column_of(octant_ref)
    for octant in range(OCTANTS):
        chosen = jnp.where(octant_of == octant, coarse_local, 0.0).astype(BF16)
        local = local + dot_rows(chosen, shift_ref[octant])

    harmonics = 16
    side = out_ref.shape[1]
    for row in range(harmonics):
        first = row * harmonics
        block = local[:, first // side * side : first // side * side + side]
        if first % side:
            block = pltpu.roll(block, side - first % side, 1)
        staged[pl.ds(row, LEAVES, stride=harmonics), :] = block
    spread = dot(jnp.concatenate(halves(staged[...]), axis=1), right_ref[...])
    spread = spread[:, :side] + spread[:, side:]
    left = left_ref[...]
    for pair in range(out_ref.shape[0] // 2):
        parts = []
        for tile in (2 * pair, 2 * pair + 1):
            tile_high, tile_low = halves(spread[tile * LEAVES : (tile + 1) * LEAVES])
            parts.append(jnp.concatenate([tile_high, tile_low, tile_high, tile_low], axis=0))
        far = dot(left, jnp.concatenate(parts, axis=1))
        for half, tile in enumerate((2 * pair, 2 * pair + 1)):
            out_ref[tile] = (near_ref[tile] + far[:, half * side : (half + 1) * side]).astype(BF16)


VMEM = pl.BlockSpec(memory_space=pltpu.VMEM)
SMEM = pl.BlockSpec(memory_space=pltpu.SMEM)
HBM = pl.BlockSpec(memory_space=pltpu.HBM)


def ready_call(*operands):
    density, kinds = operands[4:6]
    tiles, side, _ = density.shape
    return pl.pallas_call(
        ready_kernel,
        name="ready",
        out_shape=(
            jax.ShapeDtypeStruct((tiles, side, side), F32),
            jax.ShapeDtypeStruct((3, OPS * LEAVES, BLOCKS), BF16),
            jax.ShapeDtypeStruct((side, 4 * LEAVES), BF16),
            jax.ShapeDtypeStruct((2 * side, 2 * side), BF16),
        ),
        in_specs=[SMEM] * 4 + [VMEM] * 6,
        out_specs=(VMEM,) * 4,
        scratch_shapes=[pltpu.VMEM((tiles, kinds.shape[0], side, side), F32)],
        compiler_params=pltpu.CompilerParams(vmem_limit_bytes=67043328 - 4 * MIB // 2),
        cost_estimate=pl.CostEstimate(
            flops=8 * 10**9, bytes_accessed=6 * MIB, transcendentals=0
        ),
    )(*operands)


def payload_call(peers, *operands):
    return pl.pallas_call(
        payload_kernel,
        name="payload",
        out_shape=jax.ShapeDtypeStruct((peers, ROWS, HALF), BF16),
        in_specs=[HBM] * len(operands),
        out_specs=HBM,
        scratch_shapes=[pltpu.VMEM(operand.shape, operand.dtype) for operand in operands]
        + [
            pltpu.VMEM((ROWS, HALF), BF16),
            pltpu.SemaphoreType.DMA((len(operands),)),
            pltpu.SemaphoreType.DMA((2, peers)),
        ],
        compiler_params=pltpu.CompilerParams(vmem_limit_bytes=67043328),
        cost_estimate=pl.CostEstimate(
            flops=10**9, bytes_accessed=MIB, transcendentals=0
        ),
    )(*operands)


def parent_call(own, gathered, shift_up):
    return pl.pallas_call(
        parent_kernel,
        name="parents",
        out_shape=(
            jax.ShapeDtypeStruct((PARENTS + BLOCKS, COEFFS), BF16),
            jax.ShapeDtypeStruct((PARENTS, COEFFS), BF16),
        ),
        in_specs=[SMEM, VMEM, VMEM],
        out_specs=(VMEM, VMEM),
        compiler_params=pltpu.CompilerParams(vmem_limit_bytes=12 * MIB),
        cost_estimate=pl.CostEstimate(
            flops=2 * 10**9, bytes_accessed=2 * MIB, transcendentals=0
        ),
    )(own, gathered, shift_up)


def coarse_call(*operands):
    rows = OPS * LEAVES
    return pl.pallas_call(
        coarse_kernel,
        name="coarse",
        out_shape=(
            jax.ShapeDtypeStruct((rows, COEFFS), F32),
            jax.ShapeDtypeStruct((PSLOTS * LEAVES, 5 * PARENTS), BF16),
            jax.ShapeDtypeStruct((rows, PSLOTS * LEAVES), BF16),
        ),
        in_specs=[SMEM] + [VMEM] * (len(operands) - 1),
        out_specs=(VMEM, VMEM, VMEM),
        compiler_params=pltpu.CompilerParams(vmem_limit_bytes=16 * MIB),
        cost_estimate=pl.CostEstimate(
            flops=1000000000, bytes_accessed=4 * MIB, transcendentals=0
        ),
    )(*operands)


def leaf_call(*operands):
    return pl.pallas_call(
        leaf_kernel,
        name="leaf",
        out_shape=jax.ShapeDtypeStruct((LEAVES, COEFFS), F32),
        in_specs=[VMEM] * len(operands),
        out_specs=VMEM,
        compiler_params=pltpu.CompilerParams(vmem_limit_bytes=16 * MIB),
        cost_estimate=pl.CostEstimate(
            flops=10**9, bytes_accessed=4 * MIB, transcendentals=0
        ),
    )(*operands)


def final_call(*operands):
    near = operands[-1]
    return pl.pallas_call(
        final_kernel,
        name="final",
        out_shape=jax.ShapeDtypeStruct(near.shape, BF16),
        in_specs=[VMEM] * len(operands),
        out_specs=VMEM,
        scratch_shapes=[pltpu.VMEM((LEAVES * 16, near.shape[1]), F32)],
        compiler_params=pltpu.CompilerParams(vmem_limit_bytes=20 * MIB),
        cost_estimate=pl.CostEstimate(
            flops=4 * 10**9, bytes_accessed=8 * MIB, transcendentals=0
        ),
    )(*operands)


def routed(value, axis, to_even, to_odd):
    peers = lax.axis_size(axis)
    route = [(i, (i + (to_odd if i % 2 else to_even)) % peers) for i in range(peers)]
    return lax.ppermute(value, axis, route)


def body(
    leaf_moments,
    leaf_list,
    leaf_op,
    leaf_parent,
    leaf_octant,
    parent_list,
    parent_op,
    operators,
    shift_up,
    density,
    nearby_coulomb_kernel,
    near_src,
    near_kind,
    near_count,
    eval_rows,
    eval_cols,
):
    own = lax.axis_index("yz").astype(jnp.int32).reshape(1)
    parity = (lax.axis_index("gx") % 2).astype(jnp.int32).reshape(1)
    sent = payload_call(
        lax.axis_size("yz"),
        leaf_moments.reshape(LEAVES, COEFFS),
        leaf_parent,
        leaf_octant,
        parent_list[0],
        parent_op[0],
    )
    gathered = lax.all_to_all(sent, "yz", split_axis=0, concat_axis=0, tiled=True)

    near, counts, left, right = ready_call(
        parity,
        near_src,
        near_kind,
        near_count,
        density,
        nearby_coulomb_kernel,
        leaf_list.reshape(LEAVES, SLOTS),
        leaf_op.reshape(LEAVES, SLOTS),
        eval_rows.T,
        eval_cols,
    )

    window, parents = parent_call(own, gathered, shift_up)
    near1 = routed(window, "gx", -1, 1)
    far2 = routed(parents, "gx", -2, 2)
    near2 = routed(parents, "gx", 2, -2)
    mate = routed(window, "gx", 1, -1)
    leaf, hits, masks = coarse_call(
        parity, leaf_parent, gathered, window, counts
    )
    local = leaf_call(counts, leaf, near1, mate, operators)
    return final_call(
        leaf_octant,
        local,
        hits,
        masks,
        window,
        near2,
        near1,
        mate,
        far2,
        operators,
        shift_up,
        left,
        right,
        near,
    )


def solution(mesh):
    in_specs = (
        P("gx", "yz", None),
        P("gx", "yz", None),
        P("gx", "yz", None),
        P("gx", "yz"),
        P("gx", "yz"),
        P("gx", "yz", None),
        P("gx", "yz", None),
        P(),
        P(),
        P(("gx", "yz"), None, None),
        P(),
        P(("gx", "yz"), None),
        P(("gx", "yz"), None),
        P(("gx", "yz")),
        P(),
        P(),
    )
    out_specs = P(("gx", "yz"), None, None)
    return jax.shard_map(body, mesh=mesh, in_specs=in_specs, out_specs=out_specs, check_vma=False)
```
